32 devices in a mesh: dp: 2 (over x), sp: 16 (over z, y, core).
Axes of the slice: x: 2, y: 2, z: 4, core: 2. Of those that a mesh axis runs over, the one named last changes fastest.
Arguments:
- x_in: bfloat16 [24576, 1024], P(('dp', 'sp')), parts along dimension 0
- w_q: bfloat16 [1024, 1024], replicated
- w_k: bfloat16 [1024, 1024], replicated
- w_v: bfloat16 [1024, 1024], replicated
- w_o: bfloat16 [1024, 1024], replicated
- dy_in: bfloat16 [24576, 1024], P(('dp', 'sp')), parts along dimension 0
Outputs:
- output 1: bfloat16 [24576, 1024], P(('dp', 'sp')), parts along dimension 0
- output 2: bfloat16 [24576, 1024], P(('dp', 'sp')), parts along dimension 0
- output 3: float32 [2048, 1024], P('dp'), parts along dimension 0
- output 4: float32 [2048, 1024], P('dp'), parts along dimension 0
- output 5: float32 [2048, 1024], P('dp'), parts along dimension 0
- output 6: float32 [2048, 1024], P('dp'), parts along dimension 0
There are 2 independent parts. The reference program is written for one: setup_inputs(seed, part) draws one part's arguments, and reference() takes and returns one part's arrays. A program takes and returns all parts, laid end to end along the dimension named above; an argument that names none is the same for every part.
All inputs are finite; a program needn't handle non-finite values.
Results may differ from the reference program's by a relative error of at most 0.0125486.
Values are sent between devices in bfloat16 or wider.
A program may use at most 1 GiB of HBM per device.

```python
import jax
import jax.numpy as jnp
from jax import lax

D = 1024
HEADS = 16
HEAD = 64
TOKENS_DEV = 768
SP = 16
TOKENS = SP * TOKENS_DEV
DILATIONS = (1, 2, 4, 8)


def setup_inputs(seed: int = 0, part: int = 0) -> dict:
    root_key = jax.random.key(seed)
    sub_keys = jax.random.split(root_key, 6)
    x_key = jax.random.fold_in(sub_keys[0], part)
    dy_key = jax.random.fold_in(sub_keys[1], part)
    in_scale = D ** -0.5
    out_scale = (TOKENS_DEV / (4.0 * D)) ** 0.5
    x_in = jax.random.normal(x_key, (TOKENS, D), jnp.float32)
    dy_in = jax.random.normal(dy_key, (TOKENS, D), jnp.float32)
    w_q = jax.random.normal(sub_keys[2], (D, D), jnp.float32) * in_scale
    w_k = jax.random.normal(sub_keys[3], (D, D), jnp.float32) * in_scale
    w_v = jax.random.normal(sub_keys[4], (D, D), jnp.float32) * in_scale
    w_o = jax.random.normal(sub_keys[5], (D, D), jnp.float32) * out_scale
    return {'x_in': x_in.astype(jnp.bfloat16), 'w_q': w_q.astype(jnp.bfloat16), 'w_k': w_k.astype(jnp.bfloat16), 'w_v': w_v.astype(jnp.bfloat16), 'w_o': w_o.astype(jnp.bfloat16), 'dy_in': dy_in.astype(jnp.bfloat16)}


def project(left_rows, weight):
    return jnp.dot(left_rows, weight, preferred_element_type=jnp.float32).astype(jnp.bfloat16)


def pick_rows(values, dilation, seg_len):
    split_view = values.reshape(TOKENS // seg_len, seg_len // dilation, dilation, HEADS // dilation, dilation, HEAD)
    return jnp.stack([split_view[:, :, residue, :, residue, :] for residue in range(dilation)], axis=3)


def segment_attention(blocks):
    q_seg, k_seg, v_seg = blocks
    logits = jnp.einsum('iacd,jacd->acij', q_seg, k_seg)
    row_max = lax.stop_gradient(jnp.max(logits, axis=-1, keepdims=True))
    exp_logits = jnp.exp(logits - row_max)
    row_sum = jnp.sum(exp_logits, axis=-1, keepdims=True)
    seg_out = jnp.einsum('acij,jacd->iacd', exp_logits / row_sum, v_seg)
    seg_lse = jnp.transpose((row_max + jnp.log(row_sum))[..., 0], (2, 0, 1))
    return seg_out, seg_lse


def attention_core(q_f, k_f, v_f):
    q_scaled = q_f * HEAD ** -0.5
    branch_outs = []
    branch_lses = []
    for dilation in DILATIONS:
        seg_len = TOKENS_DEV * dilation // 2
        picked = (pick_rows(q_scaled, dilation, seg_len), pick_rows(k_f, dilation, seg_len), pick_rows(v_f, dilation, seg_len))
        seg_out, seg_lse = lax.map(jax.checkpoint(segment_attention), picked)
        eye_f = jnp.eye(dilation, dtype=q_f.dtype)
        eye_b = jnp.eye(dilation, dtype=bool)
        spread = seg_out[:, :, None] * eye_f[None, None, :, None, :, None]
        branch_outs.append(spread.reshape(TOKENS, HEADS, HEAD))
        lse_spread = jnp.where(eye_b[None, None, :, None, :], seg_lse[:, :, None], -jnp.inf)
        branch_lses.append(lse_spread.reshape(TOKENS, HEADS))
    lse_stack = jnp.stack(branch_lses)
    lse_max = lax.stop_gradient(jnp.max(lse_stack, axis=0))
    branch_w = jnp.exp(lse_stack - lse_max)
    merged = jnp.sum(branch_w[..., None] * jnp.stack(branch_outs), axis=0) / jnp.sum(branch_w, axis=0)[..., None]
    return merged.reshape(TOKENS, D)


def reference(x_in, w_q, w_k, w_v, w_o, dy_in):
    q_rows = project(x_in, w_q)
    k_rows = project(x_in, w_k)
    v_rows = project(x_in, w_v)
    attn_out, core_vjp = jax.vjp(attention_core, q_rows.astype(jnp.float32), k_rows.astype(jnp.float32), v_rows.astype(jnp.float32))
    attn_b = attn_out.astype(jnp.bfloat16)
    y_out = project(attn_b, w_o)
    d_attn = project(dy_in, w_o.T)
    grad_q, grad_k, grad_v = core_vjp(d_attn.astype(jnp.float32))
    dq_b = grad_q.astype(jnp.bfloat16)
    dk_b = grad_k.astype(jnp.bfloat16)
    dv_b = grad_v.astype(jnp.bfloat16)
    dx_sum = jnp.dot(dq_b, w_q.T, preferred_element_type=jnp.float32) + jnp.dot(dk_b, w_k.T, preferred_element_type=jnp.float32) + jnp.dot(dv_b, w_v.T, preferred_element_type=jnp.float32)
    dx_out = dx_sum.astype(jnp.bfloat16)
    dw_q = jnp.dot(x_in.T, dq_b, preferred_element_type=jnp.float32)
    dw_k = jnp.dot(x_in.T, dk_b, preferred_element_type=jnp.float32)
    dw_v = jnp.dot(x_in.T, dv_b, preferred_element_type=jnp.float32)
    dw_o = jnp.dot(attn_b.T, dy_in, preferred_element_type=jnp.float32)
    return y_out, dx_out, dw_q, dw_k, dw_v, dw_o
```

```python
import functools

import jax
import jax.numpy as jnp
from jax import lax
from jax.experimental import pallas as pl
from jax.experimental.pallas import tpu as pltpu
from jax.sharding import PartitionSpec as P

BF = jnp.bfloat16
F32 = jnp.float32
T = 768
D = 1024
CH = 96
NK = 384
ORDER = (0, 4, 2, 6, 1, 5, 3, 7)
NT = (((1,), (1,)), ((), ()))


def dot(a, b):
    return jnp.dot(a, b, preferred_element_type=F32)


def dot_nt(a, b):
    return lax.dot_general(a, b, NT, preferred_element_type=F32)


def perm_matrix(inverse):
    a = lax.broadcasted_iota(jnp.int32, (128, 128), 1 if inverse else 0)
    b = lax.broadcasted_iota(jnp.int32, (128, 128), 0 if inverse else 1)
    c = a // 16
    res = 4 * (c % 2) + 2 * ((c // 2) % 2) + c // 4
    src = (a % 16) * 8 + res
    return jnp.where(src == b, 1.0, 0.0).astype(BF)


def permute_into(src_ref, dst_ref):
    m = perm_matrix(False)
    for blk in range(T // 128):
        z = dot(m, src_ref[blk * 128:(blk + 1) * 128, :]).astype(BF)
        for c in range(8):
            dst_ref[c * CH + blk * 16:c * CH + blk * 16 + 16, :] = z[c * 16:c * 16 + 16, :]


def unpermute_into(src_ref, dst_ref):
    m = perm_matrix(True)
    for blk in range(T // 128):
        z = jnp.concatenate([src_ref[c * CH + blk * 16:c * CH + blk * 16 + 16, :] for c in range(8)], axis=0)
        dst_ref[blk * 128:(blk + 1) * 128, :] = dot(m, z).astype(BF)


def starts(p):
    return 2 * (p % 2), 2 * (p % 2) + (p // 2) % 2


def left_lanes(n):
    return lax.broadcasted_iota(jnp.int32, (n, 128), 1) < 64


def project_kernel(x_ref, dy_ref, wq_ref, wk_ref, wv_ref, wo_ref, xp_ref, xt_ref, dyp_ref, q_ref, k_ref, v_ref, do_ref, sel_ref):
    j = pl.program_id(0)

    @pl.when(j == 0)
    def _():
        permute_into(x_ref, xp_ref)
        permute_into(dy_ref, dyp_ref)
        for i in range(8):
            xt_ref[128 * i:128 * i + 128, :] = xp_ref[:, 128 * i:128 * i + 128].T

    q_ref[...] = (dot(xp_ref[...], wq_ref[...]).astype(BF) * 0.125).astype(BF)
    k_ref[...] = dot(xp_ref[...], wk_ref[...]).astype(BF)
    v_ref[...] = dot(xp_ref[...], wv_ref[...]).astype(BF)
    do_ref[...] = dot_nt(dyp_ref[...], wo_ref[...]).astype(BF)
    for i in range(2):
        s4, s8 = starts(2 * j + i)
        cols = slice(128 * i, 128 * i + 128)
        for which, src in enumerate((k_ref, v_ref)):
            for first, n, at in ((s4, 192, 0), (s8, 96, 192)):
                even = src[pl.ds(pl.multiple_of(first * CH, CH), n), cols]
                odd = src[pl.ds(pl.multiple_of(first * CH + NK, CH), n), cols]
                sel_ref[which, at:at + n, cols] = jnp.where(left_lanes(n), even, odd)


def project(x, dy, wq, wk, wv, wo):
    full = pl.BlockSpec((T, D), lambda j: (0, 0))
    wcol = pl.BlockSpec((D, 256), lambda j: (0, j))
    wrow = pl.BlockSpec((256, D), lambda j: (j, 0))
    tcol = pl.BlockSpec((T, 256), lambda j: (0, j))
    tok = jax.ShapeDtypeStruct((T, D), BF)
    return pl.pallas_call(
        project_kernel, grid=(4,), name='project',
        in_specs=[full, full, wcol, wcol, wcol, wrow],
        out_specs=[full, pl.BlockSpec((D, T), lambda j: (0, 0)), full, tcol, tcol, tcol, tcol, pl.BlockSpec((2, 288, 256), lambda j: (0, 0, j))],
        out_shape=[tok, jax.ShapeDtypeStruct((D, T), BF), tok, tok, tok, tok, tok, jax.ShapeDtypeStruct((2, 288, D), BF)],
        compiler_params=pltpu.CompilerParams(vmem_limit_bytes=56 << 20),
        cost_estimate=pl.CostEstimate(flops=6_500_000_000, bytes_accessed=24_000_000, transcendentals=0),
    )(x, dy, wq, wk, wv, wo)


def attention_kernel(q_ref, k_ref, v_ref, do_ref, h1_ref, h2_ref, h3_ref,
                     at_ref, dq_ref, dk_ref, dv_ref, r1_ref, r2_ref, r3_ref,
                     e_ref, m_ref, acc_ref, dqa_ref, de_ref):
    p = pl.program_id(0)
    s4, s8 = starts(p)
    left = left_lanes(NK)

    def rows_of(ref, first, n):
        return ref[pl.ds(first, n // CH)].reshape(n, ref.shape[-1])

    def pick(ref, b):
        if b < 2:
            return ref[:, b].reshape(NK, 128)
        first, n = BLOCKS[b]
        return jnp.where(left[:n], rows_of(ref, first, n), rows_of(ref, first + 4, n))

    BLOCKS = {0: (None, NK), 1: (None, NK), 2: (0, NK), 3: (s4, 192), 4: (s8, 96)}
    OFFS = (0, 384, 768, 1152, 1344)

    def keys(ref, which, b):
        own = pick(ref, b)
        if b < 3:
            return own
        if b == 3:
            return jnp.concatenate([own, h1_ref[which, 0:192, :]], axis=0)
        return jnp.concatenate([own, h1_ref[which, 192:288, :], h2_ref[which], h3_ref[which]], axis=0)

    def get(ref, e, b):
        w = ref.shape[-1]
        if b < 2:
            return ref[e, :, b].reshape(NK, w)
        first, n = BLOCKS[b]
        return ref[e, pl.ds(first + 4 * e, n // CH)].reshape(n, w)

    def put(ref, e, b, val):
        w = ref.shape[-1]
        if b < 2:
            ref[e, :, b] = val.reshape(8, 48, w)
        else:
            first, n = BLOCKS[b]
            ref[e, pl.ds(first + 4 * e, n // CH)] = val.reshape(n // CH, 2, 48, w)

    def head(val, e):
        keep = left[:val.shape[0]] if e == 0 else jnp.logical_not(left[:val.shape[0]])
        return jnp.where(keep, val, jnp.zeros_like(val))

    def wide(val):
        return jnp.concatenate([val, val, val], axis=1)

    for b in range(5):
        n = BLOCKS[b][1]
        qs, ks = pick(q_ref, b), keys(k_ref, 0, b)
        for e in range(2):
            s = dot_nt(head(qs, e), ks)
            e_ref[e, OFFS[b]:OFFS[b] + n, :] = s
            mx = jnp.broadcast_to(jnp.max(s, axis=1, keepdims=True), (n, 128))
            if b >= 2:
                mx = jnp.maximum(mx, get(m_ref, e, b))
            put(m_ref, e, b, mx)
    ones = jnp.ones((NK, 128), BF)
    for b in range(5):
        n = BLOCKS[b][1]
        vo = jnp.concatenate([keys(v_ref, 1, b), ones], axis=1)
        for e in range(2):
            ex = jnp.exp(e_ref[e, OFFS[b]:OFFS[b] + n, :] - wide(get(m_ref, e, b)))
            e_ref[e, OFFS[b]:OFFS[b] + n, :] = ex
            o = dot(ex.astype(BF), vo)
            if b >= 2:
                o = o + get(acc_ref, e, b)
            put(acc_ref, e, b, o)
    for c in range(8):
        outs = []
        dd = do_ref[c].reshape(CH, 128).astype(F32)
        for e in range(2):
            acc = acc_ref[e, c].reshape(CH, 256)
            linv = 1.0 / acc[:, 128:]
            o = acc[:, :128] * linv
            outs.append(o)
            de = jnp.sum(head(dd * o, e), axis=1, keepdims=True)
            m_ref[e, c] = linv.reshape(2, 48, 128)
            de_ref[e, c] = jnp.broadcast_to(de, (CH, 128)).reshape(2, 48, 128)
        at_ref[c] = jnp.where(left[:CH], outs[0], outs[1]).astype(BF).reshape(2, 48, 128)
    for b in range(5):
        n = BLOCKS[b][1]
        qs, ks, dos, vs = pick(q_ref, b), keys(k_ref, 0, b), pick(do_ref, b), keys(v_ref, 1, b)
        qt, dot_t = qs.T, dos.T
        dkt, dvt = [], []
        for e in range(2):
            half = slice(64 * e, 64 * e + 64)
            pn = e_ref[e, OFFS[b]:OFFS[b] + n, :] * wide(get(m_ref, e, b))
            dp = dot_nt(head(dos, e), vs)
            ds = (pn * (dp - wide(get(de_ref, e, b)))).astype(BF)
            dvt.append(dot(dot_t[half], pn.astype(BF)))
            dkt.append(dot(qt[half], ds))
            dq = dot(ds, ks)
            if b >= 2:
                dq = dq + get(dqa_ref, e, b)
            put(dqa_ref, e, b, dq)
        for which, (parts, own_ref) in enumerate(((dkt, dk_ref), (dvt, dv_ref))):
            g = jnp.concatenate(parts, axis=0).T
            if b < 2:
                own_ref[:, b] = g.reshape(8, 48, 128)
                continue
            first = BLOCKS[b][0]
            own = g[:n]
            zero = jnp.zeros_like(own)
            c = n // CH
            shape = (c, 2, 48, 128)
            own_ref[pl.ds(first, c)] += jnp.where(left[:n], own, zero).reshape(shape)
            own_ref[pl.ds(first + 4, c)] += jnp.where(left[:n], zero, own).reshape(shape)
            if b == 3:
                r1_ref[which, 0:192, :] = g[192:]
            if b == 4:
                r1_ref[which, 192:288, :] = g[96:192]
                r2_ref[which] = g[192:288]
                r3_ref[which] = g[288:384]
    for c in range(8):
        pair = jnp.where(left[:CH], dqa_ref[0, c].reshape(CH, 128), dqa_ref[1, c].reshape(CH, 128)) * 0.125
        dq_ref[c] = pair.astype(BF).reshape(2, 48, 128)


def attention(q, k, v, do, h1, h2, h3):
    heads = D // 128
    row = pl.BlockSpec((8, 2, 48, 128), lambda p: (0, 0, 0, p))
    big = pl.BlockSpec((2, 288, 128), lambda p: (0, 0, p))
    small = pl.BlockSpec((2, 96, 128), lambda p: (0, 0, p))
    r = lambda a: a.reshape(8, 2, 48, D)
    outs = pl.pallas_call(
        attention_kernel, grid=(heads,), name='attention',
        in_specs=[row] * 4 + [big, small, small],
        out_specs=[row] * 4 + [big, small, small],
        out_shape=[jax.ShapeDtypeStruct((8, 2, 48, D), BF)] * 2 + [jax.ShapeDtypeStruct((8, 2, 48, D), F32)] * 2
        + [jax.ShapeDtypeStruct((2, 288, D), F32)] + [jax.ShapeDtypeStruct((2, 96, D), F32)] * 2,
        scratch_shapes=[pltpu.VMEM((2, 1440, NK), F32), pltpu.VMEM((2, 8, 2, 48, 128), F32), pltpu.VMEM((2, 8, 2, 48, 256), F32),
                        pltpu.VMEM((2, 8, 2, 48, 128), F32), pltpu.VMEM((2, 8, 2, 48, 128), F32)],
        compiler_params=pltpu.CompilerParams(vmem_limit_bytes=56 << 20),
        cost_estimate=pl.CostEstimate(flops=30_000_000_000, bytes_accessed=24_000_000, transcendentals=9_000_000),
    )(r(q), r(k), r(v), r(do), h1, h2, h3)
    at, dq, dk, dv, r1, r2, r3 = outs
    f = lambda a: a.reshape(T, D)
    return f(at), f(dq), f(dk), f(dv), r1, r2, r3


def out_kernel(at_ref, att_ref, dyp_ref, wo_ref, xt_ref, dq_ref, y_ref, dwo_ref, dwq_ref, yp_ref):
    yp_ref[...] = dot(at_ref[...], wo_ref[...]).astype(BF)
    unpermute_into(yp_ref, y_ref)
    dwo_ref[...] = dot(att_ref[...].T, dyp_ref[...])
    dwq_ref[...] = dot(xt_ref[...], dq_ref[...])


def out_stage(at, dyp, wo, xt, dq):
    full = pl.BlockSpec((T, D), lambda j: (0, 0))
    col = pl.BlockSpec((D, 256), lambda j: (0, j))
    tcol = pl.BlockSpec((T, 256), lambda j: (0, j))
    return pl.pallas_call(
        out_kernel, grid=(4,), name='out_stage',
        in_specs=[full, tcol, full, col, pl.BlockSpec((D, T), lambda j: (0, 0)), tcol],
        out_specs=[tcol, pl.BlockSpec((256, D), lambda j: (j, 0)), col],
        out_shape=[jax.ShapeDtypeStruct((T, D), BF), jax.ShapeDtypeStruct((D, D), F32), jax.ShapeDtypeStruct((D, D), F32)],
        scratch_shapes=[pltpu.VMEM((T, 256), BF)],
        compiler_params=pltpu.CompilerParams(vmem_limit_bytes=56 << 20),
        cost_estimate=pl.CostEstimate(flops=5_000_000_000, bytes_accessed=20_000_000, transcendentals=0),
    )(at, at, dyp, wo, xt, dq)


def in_kernel(dq_ref, dk_ref, dv_ref, r1_ref, r2_ref, r3_ref, xt_ref, wq_ref, wk_ref, wv_ref, dx_ref, dwk_ref, dwv_ref, acc_ref, dxp_ref, sum_ref):
    j = pl.program_id(0)
    part = dot_nt(dq_ref[...], wq_ref[...])
    for which, (own_ref, w_ref, dw_ref) in enumerate(((dk_ref, wk_ref, dwk_ref), (dv_ref, wv_ref, dwv_ref))):
        sum_ref[...] = own_ref[...]
        for i in range(2):
            s4, s8 = starts(2 * j + i)
            cols = slice(128 * i, 128 * i + 128)
            a4 = r1_ref[which, 0:192, cols]
            a8 = r1_ref[which, 192:288, cols] + r2_ref[which, :, cols] + r3_ref[which, :, cols]
            for first, n, add in ((s4, 192, a4), (s8, 96, a8)):
                keep = left_lanes(n)
                zero = jnp.zeros_like(add)
                sum_ref[pl.ds(pl.multiple_of(first * CH, CH), n), cols] += jnp.where(keep, add, zero)
                sum_ref[pl.ds(pl.multiple_of(first * CH + NK, CH), n), cols] += jnp.where(keep, zero, add)
        g = sum_ref[...].astype(BF)
        dw_ref[...] = dot(xt_ref[...], g)
        part = part + dot_nt(g, w_ref[...])

    @pl.when(j == 0)
    def _():
        acc_ref[...] = part

    @pl.when(j > 0)
    def _():
        acc_ref[...] += part

    @pl.when(j == 3)
    def _():
        dxp_ref[...] = acc_ref[...].astype(BF)
        unpermute_into(dxp_ref, dx_ref)


def in_stage(dq, dk, dv, r1, r2, r3, xt, wq, wk, wv):
    full = pl.BlockSpec((T, D), lambda j: (0, 0))
    col = pl.BlockSpec((D, 256), lambda j: (0, j))
    tcol = pl.BlockSpec((T, 256), lambda j: (0, j))
    big = pl.BlockSpec((2, 288, 256), lambda j: (0, 0, j))
    small = pl.BlockSpec((2, 96, 256), lambda j: (0, 0, j))
    return pl.pallas_call(
        in_kernel, grid=(4,), name='in_stage',
        in_specs=[tcol, tcol, tcol, big, small, small, pl.BlockSpec((D, T), lambda j: (0, 0)), col, col, col],
        out_specs=[full, col, col],
        out_shape=[jax.ShapeDtypeStruct((T, D), BF), jax.ShapeDtypeStruct((D, D), F32), jax.ShapeDtypeStruct((D, D), F32)],
        scratch_shapes=[pltpu.VMEM((T, D), F32), pltpu.VMEM((T, D), BF), pltpu.VMEM((T, 256), F32)],
        compiler_params=pltpu.CompilerParams(vmem_limit_bytes=56 << 20),
        cost_estimate=pl.CostEstimate(flops=8_000_000_000, bytes_accessed=26_000_000, transcendentals=0),
    )(dq, dk, dv, r1, r2, r3, xt, wq, wk, wv)


def solution(mesh):
    sp_size = mesh.shape['sp']

    def swap(a, bit):
        return lax.ppermute(a, 'sp', [(i, i ^ bit) for i in range(sp_size)])

    def device_step(x, w_q, w_k, w_v, w_o, dy):
        xp, xt, dyp, q, k, v, do, sel = project(x, dy, w_q, w_k, w_v, w_o)
        sel8 = sel[:, 192:288]
        h1, h2, h3 = swap(sel, 1), swap(sel8, 2), swap(sel8, 3)
        at, dq, dk, dv, r1, r2, r3 = attention(q, k, v, do, h1, h2, h3)
        r1, r2, r3 = swap(r1, 1), swap(r2, 2), swap(r3, 3)
        y, dw_o, dw_q = out_stage(at, dyp, w_o, xt, dq)
        dx, dw_k, dw_v = in_stage(dq, dk, dv, r1, r2, r3, xt, w_q, w_k, w_v)
        dw_q, dw_k, dw_v, dw_o = lax.psum((dw_q, dw_k, dw_v, dw_o), 'sp')
        return y, dx, dw_q, dw_k, dw_v, dw_o

    row_spec = P(('dp', 'sp'), None)
    full_spec = P(None, None)
    grad_spec = P('dp', None)
    return jax.shard_map(device_step, mesh=mesh, in_specs=(row_spec, full_spec, full_spec, full_spec, full_spec, row_spec), out_specs=(row_spec, row_spec, grad_spec, grad_spec, grad_spec, grad_spec), check_vma=False)
```

```python
import functools

import jax
import jax.numpy as jnp
from jax import lax
from jax.experimental import pallas as pl
from jax.experimental.pallas import tpu as pltpu
from jax.sharding import PartitionSpec as P

BF = jnp.bfloat16
F32 = jnp.float32
T = 768
D = 1024
CH = 96
NK = 384
ORDER = (0, 4, 2, 6, 1, 5, 3, 7)
NT = (((1,), (1,)), ((), ()))


def dot(a, b):
    return jnp.dot(a, b, preferred_element_type=F32)


def dot_nt(a, b):
    return lax.dot_general(a, b, NT, preferred_element_type=F32)


def perm_matrix(inverse):
    a = lax.broadcasted_iota(jnp.int32, (128, 128), 1 if inverse else 0)
    b = lax.broadcasted_iota(jnp.int32, (128, 128), 0 if inverse else 1)
    c = a // 16
    res = 4 * (c % 2) + 2 * ((c // 2) % 2) + c // 4
    src = (a % 16) * 8 + res
    return jnp.where(src == b, 1.0, 0.0).astype(BF)


def permute_into(src_ref, dst_ref):
    m = perm_matrix(False)
    for blk in range(T // 128):
        z = dot(m, src_ref[blk * 128:(blk + 1) * 128, :]).astype(BF)
        for c in range(8):
            dst_ref[c * CH + blk * 16:c * CH + blk * 16 + 16, :] = z[c * 16:c * 16 + 16, :]


def unpermute_into(src_ref, dst_ref):
    m = perm_matrix(True)
    for blk in range(T // 128):
        z = jnp.concatenate([src_ref[c * CH + blk * 16:c * CH + blk * 16 + 16, :] for c in range(8)], axis=0)
        dst_ref[blk * 128:(blk + 1) * 128, :] = dot(m, z).astype(BF)


def starts(p):
    return 2 * (p % 2), 2 * (p % 2) + (p // 2) % 2


def left_lanes(n):
    return lax.broadcasted_iota(jnp.int32, (n, 128), 1) < 64


def project_kernel(x_ref, dy_ref, wq_ref, wk_ref, wv_ref, wo_ref, xp_ref, xt_ref, dyp_ref, q_ref, k_ref, v_ref, do_ref, sel_ref):
    j = pl.program_id(0)

    @pl.when(j == 0)
    def _():
        permute_into(x_ref, xp_ref)
        permute_into(dy_ref, dyp_ref)
        for i in range(8):
            xt_ref[128 * i:128 * i + 128, :] = xp_ref[:, 128 * i:128 * i + 128].T

    q_ref[...] = (dot(xp_ref[...], wq_ref[...]).astype(BF) * 0.125).astype(BF)
    k_ref[...] = dot(xp_ref[...], wk_ref[...]).astype(BF)
    v_ref[...] = dot(xp_ref[...], wv_ref[...]).astype(BF)
    do_ref[...] = dot_nt(dyp_ref[...], wo_ref[...]).astype(BF)
    for i in range(2):
        s4, s8 = starts(2 * j + i)
        cols = slice(128 * i, 128 * i + 128)
        for which, src in enumerate((k_ref, v_ref)):
            for first, n, at in ((s4, 192, 0), (s8, 96, 192)):
                even = src[pl.ds(pl.multiple_of(first * CH, CH), n), cols]
                odd = src[pl.ds(pl.multiple_of(first * CH + NK, CH), n), cols]
                sel_ref[which, at:at + n, cols] = jnp.where(left_lanes(n), even, odd)


def project(x, dy, wq, wk, wv, wo):
    full = pl.BlockSpec((T, D), lambda j: (0, 0))
    wcol = pl.BlockSpec((D, 256), lambda j: (0, j))
    wrow = pl.BlockSpec((256, D), lambda j: (j, 0))
    tcol = pl.BlockSpec((T, 256), lambda j: (0, j))
    tok = jax.ShapeDtypeStruct((T, D), BF)
    return pl.pallas_call(
        project_kernel, grid=(4,), name='project',
        in_specs=[full, full, wcol, wcol, wcol, wrow],
        out_specs=[full, pl.BlockSpec((D, T), lambda j: (0, 0)), full, tcol, tcol, tcol, tcol, pl.BlockSpec((2, 288, 256), lambda j: (0, 0, j))],
        out_shape=[tok, jax.ShapeDtypeStruct((D, T), BF), tok, tok, tok, tok, tok, jax.ShapeDtypeStruct((2, 288, D), BF)],
        compiler_params=pltpu.CompilerParams(vmem_limit_bytes=56 << 20),
        cost_estimate=pl.CostEstimate(flops=6_500_000_000, bytes_accessed=24_000_000, transcendentals=0),
    )(x, dy, wq, wk, wv, wo)


def attention_kernel(q_ref, k_ref, v_ref, do_ref, h1_ref, h2_ref, h3_ref,
                     at_ref, dq_ref, dk_ref, dv_ref, r1_ref, r2_ref, r3_ref,
                     e_ref, m_ref, acc_ref, dqa_ref, de_ref):
    p = pl.program_id(0)
    s4, s8 = starts(p)
    left = left_lanes(NK)

    def rows_of(ref, first, n):
        return ref[pl.ds(first, n // CH)].reshape(n, ref.shape[-1])

    def pick(ref, b):
        if b < 2:
            return ref[:, b].reshape(NK, 128)
        first, n = BLOCKS[b]
        return jnp.where(left[:n], rows_of(ref, first, n), rows_of(ref, first + 4, n))

    BLOCKS = {0: (None, NK), 1: (None, NK), 2: (0, NK), 3: (s4, 192), 4: (s8, 96)}
    OFFS = (0, 384, 768, 1152, 1344)

    def keys(ref, which, b):
        own = pick(ref, b)
        if b < 3:
            return own
        if b == 3:
            return jnp.concatenate([own, h1_ref[which, 0:192, :]], axis=0)
        return jnp.concatenate([own, h1_ref[which, 192:288, :], h2_ref[which], h3_ref[which]], axis=0)

    def get(ref, e, b):
        w = ref.shape[-1]
        if b < 2:
            return ref[e, :, b].reshape(NK, w)
        first, n = BLOCKS[b]
        return ref[e, pl.ds(first + 4 * e, n // CH)].reshape(n, w)

    def put(ref, e, b, val):
        w = ref.shape[-1]
        if b < 2:
            ref[e, :, b] = val.reshape(8, 48, w)
        else:
            first, n = BLOCKS[b]
            ref[e, pl.ds(first + 4 * e, n // CH)] = val.reshape(n // CH, 2, 48, w)

    def head(val, e):
        keep = left[:val.shape[0]] if e == 0 else jnp.logical_not(left[:val.shape[0]])
        return jnp.where(keep, val, jnp.zeros_like(val))

    def wide(val):
        return jnp.concatenate([val, val, val], axis=1)

    for b in range(5):
        n = BLOCKS[b][1]
        qs, ks = pick(q_ref, b), keys(k_ref, 0, b)
        for e in range(2):
            s = dot_nt(head(qs, e), ks)
            e_ref[e, OFFS[b]:OFFS[b] + n, :] = s
            mx = jnp.broadcast_to(jnp.max(s, axis=1, keepdims=True), (n, 128))
            if b >= 2:
                mx = jnp.maximum(mx, get(m_ref, e, b))
            put(m_ref, e, b, mx)
    ones = jnp.ones((NK, 128), BF)
    for b in range(5):
        n = BLOCKS[b][1]
        vo = jnp.concatenate([keys(v_ref, 1, b), ones], axis=1)
        for e in range(2):
            ex = jnp.exp(e_ref[e, OFFS[b]:OFFS[b] + n, :] - wide(get(m_ref, e, b)))
            e_ref[e, OFFS[b]:OFFS[b] + n, :] = ex
            o = dot(ex.astype(BF), vo)
            if b >= 2:
                o = o + get(acc_ref, e, b)
            put(acc_ref, e, b, o)
    for c in range(8):
        outs = []
        dd = do_ref[c].reshape(CH, 128).astype(F32)
        for e in range(2):
            acc = acc_ref[e, c].reshape(CH, 256)
            linv = 1.0 / acc[:, 128:]
            o = acc[:, :128] * linv
            outs.append(o)
            de = jnp.sum(head(dd * o, e), axis=1, keepdims=True)
            m_ref[e, c] = linv.reshape(2, 48, 128)
            de_ref[e, c] = jnp.broadcast_to(de, (CH, 128)).reshape(2, 48, 128)
        at_ref[c] = jnp.where(left[:CH], outs[0], outs[1]).astype(BF).reshape(2, 48, 128)
    for b in range(5):
        n = BLOCKS[b][1]
        qs, ks, dos, vs = pick(q_ref, b), keys(k_ref, 0, b), pick(do_ref, b), keys(v_ref, 1, b)
        qt, dot_t = qs.T, dos.T
        dkt, dvt = [], []
        for e in range(2):
            half = slice(64 * e, 64 * e + 64)
            pn = e_ref[e, OFFS[b]:OFFS[b] + n, :] * wide(get(m_ref, e, b))
            dp = dot_nt(head(dos, e), vs)
            ds = (pn * (dp - wide(get(de_ref, e, b)))).astype(BF)
            dvt.append(dot(dot_t[half], pn.astype(BF)))
            dkt.append(dot(qt[half], ds))
            dq = dot(ds, ks)
            if b >= 2:
                dq = dq + get(dqa_ref, e, b)
            put(dqa_ref, e, b, dq)
        for which, (parts, own_ref) in enumerate(((dkt, dk_ref), (dvt, dv_ref))):
            g = jnp.concatenate(parts, axis=0).T
            if b < 2:
                own_ref[:, b] = g.reshape(8, 48, 128)
                continue
            first = BLOCKS[b][0]
            own = g[:n]
            zero = jnp.zeros_like(own)
            c = n // CH
            shape = (c, 2, 48, 128)
            own_ref[pl.ds(first, c)] += jnp.where(left[:n], own, zero).reshape(shape)
            own_ref[pl.ds(first + 4, c)] += jnp.where(left[:n], zero, own).reshape(shape)
            if b == 3:
                r1_ref[which, 0:192, :] = g[192:]
            if b == 4:
                r1_ref[which, 192:288, :] = g[96:192]
                r2_ref[which] = g[192:288]
                r3_ref[which] = g[288:384]
    for c in range(8):
        pair = jnp.where(left[:CH], dqa_ref[0, c].reshape(CH, 128), dqa_ref[1, c].reshape(CH, 128)) * 0.125
        dq_ref[c] = pair.astype(BF).reshape(2, 48, 128)


def attention(q, k, v, do, h1, h2, h3):
    heads = D // 128
    row = pl.BlockSpec((8, 2, 48, 128), lambda p: (0, 0, 0, p))
    big = pl.BlockSpec((2, 288, 128), lambda p: (0, 0, p))
    small = pl.BlockSpec((2, 96, 128), lambda p: (0, 0, p))
    r = lambda a: a.reshape(8, 2, 48, D)
    outs = pl.pallas_call(
        attention_kernel, grid=(heads,), name='attention',
        in_specs=[row] * 4 + [big, small, small],
        out_specs=[row] * 4 + [big, small, small],
        out_shape=[jax.ShapeDtypeStruct((8, 2, 48, D), BF)] * 2 + [jax.ShapeDtypeStruct((8, 2, 48, D), F32)] * 2
        + [jax.ShapeDtypeStruct((2, 288, D), F32)] + [jax.ShapeDtypeStruct((2, 96, D), F32)] * 2,
        scratch_shapes=[pltpu.VMEM((2, 1440, NK), F32), pltpu.VMEM((2, 8, 2, 48, 128), F32), pltpu.VMEM((2, 8, 2, 48, 256), F32),
                        pltpu.VMEM((2, 8, 2, 48, 128), F32), pltpu.VMEM((2, 8, 2, 48, 128), F32)],
        compiler_params=pltpu.CompilerParams(vmem_limit_bytes=56 << 20),
        cost_estimate=pl.CostEstimate(flops=30_000_000_000, bytes_accessed=24_000_000, transcendentals=9_000_000),
    )(r(q), r(k), r(v), r(do), h1, h2, h3)
    at, dq, dk, dv, r1, r2, r3 = outs
    f = lambda a: a.reshape(T, D)
    return f(at), f(dq), f(dk), f(dv), r1, r2, r3


def out_kernel(at_ref, wo_ref, y_ref, att_ref, yp_ref):
    j = pl.program_id(0)
    yp_ref[...] = dot(at_ref[...], wo_ref[...]).astype(BF)
    unpermute_into(yp_ref, y_ref)

    @pl.when(j == 0)
    def _():
        for i in range(8):
            att_ref[128 * i:128 * i + 128, :] = at_ref[:, 128 * i:128 * i + 128].T


def out_stage(at, wo):
    full = pl.BlockSpec((T, D), lambda j: (0, 0))
    col = pl.BlockSpec((D, 256), lambda j: (0, j))
    tcol = pl.BlockSpec((T, 256), lambda j: (0, j))
    return pl.pallas_call(
        out_kernel, grid=(4,), name='out_stage',
        in_specs=[full, col],
        out_specs=[tcol, pl.BlockSpec((D, T), lambda j: (0, 0))],
        out_shape=[jax.ShapeDtypeStruct((T, D), BF), jax.ShapeDtypeStruct((D, T), BF)],
        scratch_shapes=[pltpu.VMEM((T, 256), BF)],
        compiler_params=pltpu.CompilerParams(vmem_limit_bytes=56 << 20),
        cost_estimate=pl.CostEstimate(flops=1_700_000_000, bytes_accessed=8_000_000, transcendentals=0),
    )(at, wo)


def in_kernel(dq_ref, dk_ref, dv_ref, r1_ref, r2_ref, r3_ref, wq_ref, wk_ref, wv_ref, dx_ref, dkb_ref, dvb_ref, acc_ref, dxp_ref, sum_ref):
    j = pl.program_id(0)
    part = dot_nt(dq_ref[...], wq_ref[...])
    for which, (own_ref, w_ref, g_ref) in enumerate(((dk_ref, wk_ref, dkb_ref), (dv_ref, wv_ref, dvb_ref))):
        sum_ref[...] = own_ref[...]
        for i in range(2):
            s4, s8 = starts(2 * j + i)
            cols = slice(128 * i, 128 * i + 128)
            a4 = r1_ref[which, 0:192, cols]
            a8 = r1_ref[which, 192:288, cols] + r2_ref[which, :, cols] + r3_ref[which, :, cols]
            for first, n, add in ((s4, 192, a4), (s8, 96, a8)):
                keep = left_lanes(n)
                zero = jnp.zeros_like(add)
                sum_ref[pl.ds(pl.multiple_of(first * CH, CH), n), cols] += jnp.where(keep, add, zero)
                sum_ref[pl.ds(pl.multiple_of(first * CH + NK, CH), n), cols] += jnp.where(keep, zero, add)
        g_ref[...] = sum_ref[...].astype(BF)
        part = part + dot_nt(g_ref[...], w_ref[...])

    @pl.when(j == 0)
    def _():
        acc_ref[...] = part

    @pl.when(j > 0)
    def _():
        acc_ref[...] += part

    @pl.when(j == 3)
    def _():
        dxp_ref[...] = acc_ref[...].astype(BF)
        unpermute_into(dxp_ref, dx_ref)


def in_stage(dq, dk, dv, r1, r2, r3, wq, wk, wv):
    full = pl.BlockSpec((T, D), lambda j: (0, 0))
    col = pl.BlockSpec((D, 256), lambda j: (0, j))
    tcol = pl.BlockSpec((T, 256), lambda j: (0, j))
    big = pl.BlockSpec((2, 288, 256), lambda j: (0, 0, j))
    small = pl.BlockSpec((2, 96, 256), lambda j: (0, 0, j))
    return pl.pallas_call(
        in_kernel, grid=(4,), name='in_stage',
        in_specs=[tcol, tcol, tcol, big, small, small, col, col, col],
        out_specs=[full, tcol, tcol],
        out_shape=[jax.ShapeDtypeStruct((T, D), BF)] * 3,
        scratch_shapes=[pltpu.VMEM((T, D), F32), pltpu.VMEM((T, D), BF), pltpu.VMEM((T, 256), F32)],
        compiler_params=pltpu.CompilerParams(vmem_limit_bytes=56 << 20),
        cost_estimate=pl.CostEstimate(flops=5_000_000_000, bytes_accessed=16_000_000, transcendentals=0),
    )(dq, dk, dv, r1, r2, r3, wq, wk, wv)


STEPS = 8
PAIRS = tuple((d, u) for u in range(2) for d in range(2))


def ring_kernel(xt_ref, att_ref, dq_ref, dk_ref, dv_ref, dy_ref, *refs):
    (outs, (acc, prt, stage, rs_send, rs_recv, pt_send, pt_recv, ag_send, ag_recv, cc_send, cc_recv, lo_sem)) = (refs[:4], refs[4:])
    out = ((outs[0], outs[1]), (outs[2], outs[3]))
    lhs = ((att_ref, xt_ref), (xt_ref, xt_ref))
    rhs = ((dy_ref, dq_ref), (dk_ref, dv_ref))
    s = lax.axis_index('sp')
    core, y, z = s % 2, (s // 2) % 2, s // 4
    pos = z + y * (7 - 2 * z)
    mate = {'sp': s + 1 - 2 * core}

    def member(r):
        r = r % STEPS
        row = r // 4
        return {'sp': (r + row * (7 - 2 * r)) * 4 + row * 2 + core}

    ahead = (member(pos + 1), member(pos + STEPS - 1))
    mine = pl.ds(pl.multiple_of(512 * core, 512), 512)
    other = pl.ds(pl.multiple_of(512 * (1 - core), 512), 512)

    def shard(d, step):
        return (pos + 15 - step) % STEPS if d == 0 else (pos + 1 + step) % STEPS

    def rows(i):
        return pl.ds(pl.multiple_of(128 * i, 128), 128)

    def partial(d, u, step, cols):
        return dot(lhs[d][u][rows(shard(d, step)), :], rhs[d][u][:, cols])

    def remote(src, dst, send, recv, peer):
        return pltpu.make_async_remote_copy(src_ref=src, dst_ref=dst, send_sem=send, recv_sem=recv, device_id=peer, device_id_type=pl.DeviceIdType.MESH)

    def to_mate(d, u, step):
        return remote(stage.at[d, u, step % 2], prt.at[d, u, step], pt_send.at[d, u, step], pt_recv.at[d, u, step], mate)

    def to_next(d, u, step):
        return remote(acc.at[d, u, step], acc.at[d, u, step + 1], rs_send.at[d, u, step], rs_recv.at[d, u, step], ahead[d])

    def give(d, u, step):
        stage[d, u, step % 2] = partial(d, u, step, other)
        to_mate(d, u, step).start()

    def spread(d, u, t):
        i = (pos + 8 - t) % STEPS if d == 0 else (pos + t) % STEPS
        return out[d][u].at[rows(i), mine]

    def gather_next(d, u, t, src):
        return remote(src, spread(d, u, t), ag_send.at[d, u, t], ag_recv.at[d, u, t], ahead[d])

    def gather_mate(d, u, t, src):
        return remote(src, spread(d, u, t), cc_send.at[d, u, t], cc_recv.at[d, u, t], mate)

    for d, u in PAIRS:
        give(d, u, 0)
    for d, u in PAIRS:
        acc[d, u, 0] = partial(d, u, 0, mine)
        to_mate(d, u, 0).wait_recv()
        acc[d, u, 0] += prt[d, u, 0]
        to_next(d, u, 0).start()
    for d, u in PAIRS:
        give(d, u, 1)

    def reduce_step(step, carry):
        for d, u in PAIRS:
            part = partial(d, u, step, mine)
            to_mate(d, u, step).wait_recv()
            to_next(d, u, step - 1).wait_recv()
            acc[d, u, step] += prt[d, u, step] + part
            to_next(d, u, step).start()
        for d, u in PAIRS:
            to_mate(d, u, step - 1).wait_send()
            give(d, u, step + 1)
        return carry

    lax.fori_loop(1, STEPS - 1, reduce_step, 0)
    last = STEPS - 1
    for d, u in PAIRS:
        part = partial(d, u, last, mine)
        to_mate(d, u, last).wait_recv()
        to_next(d, u, last - 1).wait_recv()
        acc[d, u, last] += prt[d, u, last] + part
        src = acc.at[d, u, last]
        gather_next(d, u, 0, src).start()
        gather_mate(d, u, 0, src).start()
        pltpu.make_async_copy(src, spread(d, u, 0), lo_sem.at[d, u]).start()

    def gather_step(t, carry):
        for d, u in PAIRS:
            gather_next(d, u, t - 1, acc.at[d, u, last]).wait_recv()
            gather_next(d, u, t, spread(d, u, t)).start()
            gather_mate(d, u, t, spread(d, u, t)).start()
        return carry

    lax.fori_loop(1, STEPS - 1, gather_step, 0)
    for d, u in PAIRS:
        gather_next(d, u, last - 1, acc.at[d, u, last]).wait_recv()
        gather_mate(d, u, last, spread(d, u, last)).start()

    def drain(t, carry):
        for d, u in PAIRS:
            to_next(d, u, t).wait_send()
            gather_next(d, u, t, acc.at[d, u, last]).wait_send()
            gather_mate(d, u, t, acc.at[d, u, last]).wait()
        return carry

    lax.fori_loop(0, last, drain, 0)
    for d, u in PAIRS:
        gather_mate(d, u, last, acc.at[d, u, last]).wait()
        to_mate(d, u, last - 1).wait_send()
        to_mate(d, u, last).wait_send()
        pltpu.make_async_copy(acc.at[d, u, last], spread(d, u, 0), lo_sem.at[d, u]).wait()


def ring_stage(xt, att, dq, dk, dv, dyp):
    sem = lambda n: pltpu.SemaphoreType.DMA((2, 2, n))
    return pl.pallas_call(
        ring_kernel, name='ring_stage',
        in_specs=[pl.BlockSpec(memory_space=pltpu.VMEM)] * 6,
        out_specs=[pl.BlockSpec(memory_space=pl.ANY)] * 4,
        out_shape=[jax.ShapeDtypeStruct((D, D), F32)] * 4,
        scratch_shapes=[pltpu.VMEM((2, 2, STEPS, 128, 512), F32), pltpu.VMEM((2, 2, STEPS, 128, 512), F32), pltpu.VMEM((2, 2, 2, 128, 512), F32),
                        sem(7), sem(7), sem(8), sem(8), sem(7), sem(7), sem(8), sem(8), pltpu.SemaphoreType.DMA((2, 2))],
        compiler_params=pltpu.CompilerParams(has_side_effects=True, vmem_limit_bytes=56 << 20),
        cost_estimate=pl.CostEstimate(flops=7_000_000_000, bytes_accessed=40_000_000, transcendentals=0),
    )(xt, att, dq, dk, dv, dyp)


def solution(mesh):
    sp_size = mesh.shape['sp']

    def swap(a, bit):
        return lax.ppermute(a, 'sp', [(i, i ^ bit) for i in range(sp_size)])

    def device_step(x, w_q, w_k, w_v, w_o, dy):
        xp, xt, dyp, q, k, v, do, sel = project(x, dy, w_q, w_k, w_v, w_o)
        sel8 = sel[:, 192:288]
        h1, h2, h3 = swap(sel, 1), swap(sel8, 2), swap(sel8, 3)
        at, dq, dk, dv, r1, r2, r3 = attention(q, k, v, do, h1, h2, h3)
        r1, r2, r3 = swap(r1, 1), swap(r2, 2), swap(r3, 3)
        y, att = out_stage(at, w_o)
        dx, dkb, dvb = in_stage(dq, dk, dv, r1, r2, r3, w_q, w_k, w_v)
        dw_o, dw_q, dw_k, dw_v = ring_stage(xt, att, dq, dkb, dvb, dyp)
        return y, dx, dw_q, dw_k, dw_v, dw_o

    row_spec = P(('dp', 'sp'), None)
    full_spec = P(None, None)
    grad_spec = P('dp', None)
    return jax.shard_map(device_step, mesh=mesh, in_specs=(row_spec, full_spec, full_spec, full_spec, full_spec, row_spec), out_specs=(row_spec, row_spec, grad_spec, grad_spec, grad_spec, grad_spec), check_vma=False)
```

```python
import functools

import jax
import jax.numpy as jnp
from jax import lax
from jax.experimental import pallas as pl
from jax.experimental.pallas import tpu as pltpu
from jax.sharding import PartitionSpec as P

BF = jnp.bfloat16
F32 = jnp.float32
T = 768
D = 1024
CH = 96
NK = 384
ORDER = (0, 4, 2, 6, 1, 5, 3, 7)
NT = (((1,), (1,)), ((), ()))


def dot(a, b):
    return jnp.dot(a, b, preferred_element_type=F32)


def dot_nt(a, b):
    return lax.dot_general(a, b, NT, preferred_element_type=F32)


def perm_matrix(inverse):
    a = lax.broadcasted_iota(jnp.int32, (128, 128), 1 if inverse else 0)
    b = lax.broadcasted_iota(jnp.int32, (128, 128), 0 if inverse else 1)
    c = a // 16
    res = 4 * (c % 2) + 2 * ((c // 2) % 2) + c // 4
    src = (a % 16) * 8 + res
    return jnp.where(src == b, 1.0, 0.0).astype(BF)


def permute_into(src_ref, dst_ref):
    m = perm_matrix(False)
    for blk in range(T // 128):
        z = dot(m, src_ref[blk * 128:(blk + 1) * 128, :]).astype(BF)
        for c in range(8):
            dst_ref[c * CH + blk * 16:c * CH + blk * 16 + 16, :] = z[c * 16:c * 16 + 16, :]


def unpermute_into(src_ref, dst_ref):
    m = perm_matrix(True)
    for blk in range(T // 128):
        z = jnp.concatenate([src_ref[c * CH + blk * 16:c * CH + blk * 16 + 16, :] for c in range(8)], axis=0)
        dst_ref[blk * 128:(blk + 1) * 128, :] = dot(m, z).astype(BF)


def starts(p):
    return 2 * (p % 2), 2 * (p % 2) + (p // 2) % 2


def left_lanes(n):
    return lax.broadcasted_iota(jnp.int32, (n, 128), 1) < 64


def project_kernel(x_ref, dy_ref, wq_ref, wk_ref, wv_ref, wo_ref, xp_ref, xt_ref, dyp_ref, q_ref, k_ref, v_ref, do_ref, sel_ref):
    j = pl.program_id(0)

    @pl.when(j == 0)
    def _():
        permute_into(x_ref, xp_ref)
        permute_into(dy_ref, dyp_ref)
        for i in range(8):
            xt_ref[128 * i:128 * i + 128, :] = xp_ref[:, 128 * i:128 * i + 128].T

    q_ref[...] = (dot(xp_ref[...], wq_ref[...]).astype(BF) * 0.125).astype(BF)
    k_ref[...] = dot(xp_ref[...], wk_ref[...]).astype(BF)
    v_ref[...] = dot(xp_ref[...], wv_ref[...]).astype(BF)
    do_ref[...] = dot_nt(dyp_ref[...], wo_ref[...]).astype(BF)
    for i in range(2):
        s4, s8 = starts(2 * j + i)
        cols = slice(128 * i, 128 * i + 128)
        for which, src in enumerate((k_ref, v_ref)):
            for first, n, at in ((s4, 192, 0), (s8, 96, 192)):
                even = src[pl.ds(pl.multiple_of(first * CH, CH), n), cols]
                odd = src[pl.ds(pl.multiple_of(first * CH + NK, CH), n), cols]
                sel_ref[which, at:at + n, cols] = jnp.where(left_lanes(n), even, odd)


def project(x, dy, wq, wk, wv, wo):
    full = pl.BlockSpec((T, D), lambda j: (0, 0))
    wcol = pl.BlockSpec((D, 256), lambda j: (0, j))
    wrow = pl.BlockSpec((256, D), lambda j: (j, 0))
    tcol = pl.BlockSpec((T, 256), lambda j: (0, j))
    tok = jax.ShapeDtypeStruct((T, D), BF)
    return pl.pallas_call(
        project_kernel, grid=(4,), name='project',
        in_specs=[full, full, wcol, wcol, wcol, wrow],
        out_specs=[full, pl.BlockSpec((D, T), lambda j: (0, 0)), full, tcol, tcol, tcol, tcol, pl.BlockSpec((2, 288, 256), lambda j: (0, 0, j))],
        out_shape=[tok, jax.ShapeDtypeStruct((D, T), BF), tok, tok, tok, tok, tok, jax.ShapeDtypeStruct((2, 288, D), BF)],
        compiler_params=pltpu.CompilerParams(vmem_limit_bytes=56 << 20),
        cost_estimate=pl.CostEstimate(flops=6_500_000_000, bytes_accessed=24_000_000, transcendentals=0),
    )(x, dy, wq, wk, wv, wo)


def attention_kernel(q_ref, k_ref, v_ref, do_ref, h1_ref, h2_ref, h3_ref,
                     at_ref, dq_ref, dk_ref, dv_ref, r1_ref, r2_ref, r3_ref,
                     e_ref, m_ref, acc_ref, dqa_ref, de_ref):
    p = pl.program_id(0)
    s4, s8 = starts(p)
    left = left_lanes(NK)

    def rows_of(ref, first, n):
        return ref[pl.ds(first, n // CH)].reshape(n, ref.shape[-1])

    def pick(ref, b):
        if b < 2:
            return ref[:, b].reshape(NK, 128)
        first, n = BLOCKS[b]
        return jnp.where(left[:n], rows_of(ref, first, n), rows_of(ref, first + 4, n))

    BLOCKS = {0: (None, NK), 1: (None, NK), 2: (0, NK), 3: (s4, 192), 4: (s8, 96)}
    OFFS = (0, 384, 768, 1152, 1344)

    def keys(ref, which, b):
        own = pick(ref, b)
        if b < 3:
            return own
        if b == 3:
            return jnp.concatenate([own, h1_ref[which, 0:192, :]], axis=0)
        return jnp.concatenate([own, h1_ref[which, 192:288, :], h2_ref[which], h3_ref[which]], axis=0)

    def get(ref, e, b):
        w = ref.shape[-1]
        if b < 2:
            return ref[e, :, b].reshape(NK, w)
        first, n = BLOCKS[b]
        return ref[e, pl.ds(first + 4 * e, n // CH)].reshape(n, w)

    def put(ref, e, b, val):
        w = ref.shape[-1]
        if b < 2:
            ref[e, :, b] = val.reshape(8, 48, w)
        else:
            first, n = BLOCKS[b]
            ref[e, pl.ds(first + 4 * e, n // CH)] = val.reshape(n // CH, 2, 48, w)

    def head(val, e):
        keep = left[:val.shape[0]] if e == 0 else jnp.logical_not(left[:val.shape[0]])
        return jnp.where(keep, val, jnp.zeros_like(val))

    def wide(val):
        return jnp.concatenate([val, val, val], axis=1)

    for b in range(5):
        n = BLOCKS[b][1]
        qs, ks = pick(q_ref, b), keys(k_ref, 0, b)
        for e in range(2):
            s = dot_nt(head(qs, e), ks)
            e_ref[e, OFFS[b]:OFFS[b] + n, :] = s
            mx = jnp.broadcast_to(jnp.max(s, axis=1, keepdims=True), (n, 128))
            if b >= 2:
                mx = jnp.maximum(mx, get(m_ref, e, b))
            put(m_ref, e, b, mx)
    ones = jnp.ones((NK, 128), BF)
    for b in range(5):
        n = BLOCKS[b][1]
        vo = jnp.concatenate([keys(v_ref, 1, b), ones], axis=1)
        for e in range(2):
            ex = jnp.exp(e_ref[e, OFFS[b]:OFFS[b] + n, :] - wide(get(m_ref, e, b)))
            e_ref[e, OFFS[b]:OFFS[b] + n, :] = ex
            o = dot(ex.astype(BF), vo)
            if b >= 2:
                o = o + get(acc_ref, e, b)
            put(acc_ref, e, b, o)
    for c in range(8):
        outs = []
        dd = do_ref[c].reshape(CH, 128).astype(F32)
        for e in range(2):
            acc = acc_ref[e, c].reshape(CH, 256)
            linv = 1.0 / acc[:, 128:]
            o = acc[:, :128] * linv
            outs.append(o)
            de = jnp.sum(head(dd * o, e), axis=1, keepdims=True)
            m_ref[e, c] = linv.reshape(2, 48, 128)
            de_ref[e, c] = jnp.broadcast_to(de, (CH, 128)).reshape(2, 48, 128)
        at_ref[c] = jnp.where(left[:CH], outs[0], outs[1]).astype(BF).reshape(2, 48, 128)
    for b in range(5):
        n = BLOCKS[b][1]
        qs, ks, dos, vs = pick(q_ref, b), keys(k_ref, 0, b), pick(do_ref, b), keys(v_ref, 1, b)
        qt, dot_t = qs.T, dos.T
        dkt, dvt = [], []
        for e in range(2):
            half = slice(64 * e, 64 * e + 64)
            pn = e_ref[e, OFFS[b]:OFFS[b] + n, :] * wide(get(m_ref, e, b))
            dp = dot_nt(head(dos, e), vs)
            ds = (pn * (dp - wide(get(de_ref, e, b)))).astype(BF)
            dvt.append(dot(dot_t[half], pn.astype(BF)))
            dkt.append(dot(qt[half], ds))
            dq = dot(ds, ks)
            if b >= 2:
                dq = dq + get(dqa_ref, e, b)
            put(dqa_ref, e, b, dq)
        for which, (parts, own_ref) in enumerate(((dkt, dk_ref), (dvt, dv_ref))):
            g = jnp.concatenate(parts, axis=0).T
            if b < 2:
                own_ref[:, b] = g.reshape(8, 48, 128)
                continue
            first = BLOCKS[b][0]
            own = g[:n]
            zero = jnp.zeros_like(own)
            c = n // CH
            shape = (c, 2, 48, 128)
            own_ref[pl.ds(first, c)] += jnp.where(left[:n], own, zero).reshape(shape)
            own_ref[pl.ds(first + 4, c)] += jnp.where(left[:n], zero, own).reshape(shape)
            if b == 3:
                r1_ref[which, 0:192, :] = g[192:]
            if b == 4:
                r1_ref[which, 192:288, :] = g[96:192]
                r2_ref[which] = g[192:288]
                r3_ref[which] = g[288:384]
    for c in range(8):
        pair = jnp.where(left[:CH], dqa_ref[0, c].reshape(CH, 128), dqa_ref[1, c].reshape(CH, 128)) * 0.125
        dq_ref[c] = pair.astype(BF).reshape(2, 48, 128)


def attention(q, k, v, do, h1, h2, h3):
    heads = D // 128
    row = pl.BlockSpec((8, 2, 48, 128), lambda p: (0, 0, 0, p))
    big = pl.BlockSpec((2, 288, 128), lambda p: (0, 0, p))
    small = pl.BlockSpec((2, 96, 128), lambda p: (0, 0, p))
    r = lambda a: a.reshape(8, 2, 48, D)
    outs = pl.pallas_call(
        attention_kernel, grid=(heads,), name='attention',
        in_specs=[row] * 4 + [big, small, small],
        out_specs=[row] * 4 + [big, small, small],
        out_shape=[jax.ShapeDtypeStruct((8, 2, 48, D), BF)] * 2 + [jax.ShapeDtypeStruct((8, 2, 48, D), F32)] * 2
        + [jax.ShapeDtypeStruct((2, 288, D), F32)] + [jax.ShapeDtypeStruct((2, 96, D), F32)] * 2,
        scratch_shapes=[pltpu.VMEM((2, 1440, NK), F32), pltpu.VMEM((2, 8, 2, 48, 128), F32), pltpu.VMEM((2, 8, 2, 48, 256), F32),
                        pltpu.VMEM((2, 8, 2, 48, 128), F32), pltpu.VMEM((2, 8, 2, 48, 128), F32)],
        compiler_params=pltpu.CompilerParams(vmem_limit_bytes=56 << 20),
        cost_estimate=pl.CostEstimate(flops=30_000_000_000, bytes_accessed=24_000_000, transcendentals=9_000_000),
    )(r(q), r(k), r(v), r(do), h1, h2, h3)
    at, dq, dk, dv, r1, r2, r3 = outs
    f = lambda a: a.reshape(T, D)
    return f(at), f(dq), f(dk), f(dv), r1, r2, r3


def out_kernel(at_ref, wo_ref, dq_ref, wq_ref, y_ref, att_ref, dxq_ref, yp_ref):
    j = pl.program_id(0)
    yp_ref[...] = dot(at_ref[...], wo_ref[...]).astype(BF)
    unpermute_into(yp_ref, y_ref)
    part = dot_nt(dq_ref[...], wq_ref[...])

    @pl.when(j == 0)
    def _():
        dxq_ref[...] = part

    @pl.when(j > 0)
    def _():
        dxq_ref[...] += part

    @pl.when(j == 0)
    def _():
        for i in range(8):
            att_ref[128 * i:128 * i + 128, :] = at_ref[:, 128 * i:128 * i + 128].T


def out_stage(at, wo, dq, wq):
    full = pl.BlockSpec((T, D), lambda j: (0, 0))
    col = pl.BlockSpec((D, 256), lambda j: (0, j))
    tcol = pl.BlockSpec((T, 256), lambda j: (0, j))
    return pl.pallas_call(
        out_kernel, grid=(4,), name='out_stage',
        in_specs=[full, col, tcol, col],
        out_specs=[tcol, pl.BlockSpec((D, T), lambda j: (0, 0)), full],
        out_shape=[jax.ShapeDtypeStruct((T, D), BF), jax.ShapeDtypeStruct((D, T), BF), jax.ShapeDtypeStruct((T, D), F32)],
        scratch_shapes=[pltpu.VMEM((T, 256), BF)],
        compiler_params=pltpu.CompilerParams(vmem_limit_bytes=56 << 20),
        cost_estimate=pl.CostEstimate(flops=3_300_000_000, bytes_accessed=15_000_000, transcendentals=0),
    )(at, wo, dq, wq)


def in_kernel(dxq_ref, dk_ref, dv_ref, r1_ref, r2_ref, wk_ref, wv_ref, dx_ref, dkb_ref, dvb_ref, acc_ref, dxp_ref, sum_ref):
    j = pl.program_id(0)
    part = None
    for which, (own_ref, w_ref, g_ref) in enumerate(((dk_ref, wk_ref, dkb_ref), (dv_ref, wv_ref, dvb_ref))):
        sum_ref[...] = own_ref[...]
        for i in range(2):
            s4, s8 = starts(2 * j + i)
            cols = slice(128 * i, 128 * i + 128)
            a4 = r1_ref[which, 0:192, cols]
            a8 = r1_ref[which, 192:288, cols] + r2_ref[which, :, cols]
            for first, n, add in ((s4, 192, a4), (s8, 96, a8)):
                keep = left_lanes(n)
                zero = jnp.zeros_like(add)
                sum_ref[pl.ds(pl.multiple_of(first * CH, CH), n), cols] += jnp.where(keep, add, zero)
                sum_ref[pl.ds(pl.multiple_of(first * CH + NK, CH), n), cols] += jnp.where(keep, zero, add)
        g_ref[...] = sum_ref[...].astype(BF)
        term = dot_nt(g_ref[...], w_ref[...])
        part = term if part is None else part + term

    @pl.when(j == 0)
    def _():
        acc_ref[...] = dxq_ref[...] + part

    @pl.when(j > 0)
    def _():
        acc_ref[...] += part

    @pl.when(j == 3)
    def _():
        dxp_ref[...] = acc_ref[...].astype(BF)
        unpermute_into(dxp_ref, dx_ref)


def in_stage(dxq, dk, dv, r1, r2, wk, wv):
    full = pl.BlockSpec((T, D), lambda j: (0, 0))
    col = pl.BlockSpec((D, 256), lambda j: (0, j))
    tcol = pl.BlockSpec((T, 256), lambda j: (0, j))
    big = pl.BlockSpec((2, 288, 256), lambda j: (0, 0, j))
    small = pl.BlockSpec((2, 96, 256), lambda j: (0, 0, j))
    return pl.pallas_call(
        in_kernel, grid=(4,), name='in_stage',
        in_specs=[full, tcol, tcol, big, small, col, col],
        out_specs=[full, tcol, tcol],
        out_shape=[jax.ShapeDtypeStruct((T, D), BF)] * 3,
        scratch_shapes=[pltpu.VMEM((T, D), F32), pltpu.VMEM((T, D), BF), pltpu.VMEM((T, 256), F32)],
        compiler_params=pltpu.CompilerParams(vmem_limit_bytes=56 << 20),
        cost_estimate=pl.CostEstimate(flops=5_000_000_000, bytes_accessed=16_000_000, transcendentals=0),
    )(dxq, dk, dv, r1, r2, wk, wv)


STEPS = 8
PAIRS = tuple((d, u) for u in range(2) for d in range(2))


def ring_kernel(xt_ref, att_ref, dq_ref, dk_ref, dv_ref, dy_ref, *refs):
    (outs, (acc, prt, stage, rs_send, rs_recv, pt_send, pt_recv, ag_send, ag_recv, cc_send, cc_recv, lo_sem)) = (refs[:4], refs[4:])
    out = ((outs[0], outs[1]), (outs[2], outs[3]))
    lhs = ((att_ref, xt_ref), (xt_ref, xt_ref))
    rhs = ((dy_ref, dq_ref), (dk_ref, dv_ref))
    s = lax.axis_index('sp')
    core, y, z = s % 2, (s // 2) % 2, s // 4
    pos = z + y * (7 - 2 * z)
    mate = {'sp': s + 1 - 2 * core}

    def member(r):
        r = r % STEPS
        row = r // 4
        return {'sp': (r + row * (7 - 2 * r)) * 4 + row * 2 + core}

    ahead = (member(pos + 1), member(pos + STEPS - 1))
    mine = pl.ds(pl.multiple_of(512 * core, 512), 512)
    other = pl.ds(pl.multiple_of(512 * (1 - core), 512), 512)

    def shard(d, step):
        return (pos + 15 - step) % STEPS if d == 0 else (pos + 1 + step) % STEPS

    def rows(i):
        return pl.ds(pl.multiple_of(128 * i, 128), 128)

    def partial(d, u, step, cols):
        return dot(lhs[d][u][rows(shard(d, step)), :], rhs[d][u][:, cols])

    def remote(src, dst, send, recv, peer):
        return pltpu.make_async_remote_copy(src_ref=src, dst_ref=dst, send_sem=send, recv_sem=recv, device_id=peer, device_id_type=pl.DeviceIdType.MESH)

    def to_mate(d, u, step):
        return remote(stage.at[d, u, step % 2], prt.at[d, u, step], pt_send.at[d, u, step], pt_recv.at[d, u, step], mate)

    def to_next(d, u, step):
        return remote(acc.at[d, u, step], acc.at[d, u, step + 1], rs_send.at[d, u, step], rs_recv.at[d, u, step], ahead[d])

    def give(d, u, step):
        stage[d, u, step % 2] = partial(d, u, step, other)
        to_mate(d, u, step).start()

    def spread(d, u, t):
        i = (pos + 8 - t) % STEPS if d == 0 else (pos + t) % STEPS
        return out[d][u].at[rows(i), mine]

    def gather_next(d, u, t, src):
        return remote(src, spread(d, u, t), ag_send.at[d, u, t], ag_recv.at[d, u, t], ahead[d])

    def gather_mate(d, u, t, src):
        return remote(src, spread(d, u, t), cc_send.at[d, u, t], cc_recv.at[d, u, t], mate)

    for d, u in PAIRS:
        give(d, u, 0)
    for d, u in PAIRS:
        acc[d, u, 0] = partial(d, u, 0, mine)
        to_mate(d, u, 0).wait_recv()
        acc[d, u, 0] += prt[d, u, 0]
        to_next(d, u, 0).start()
    for d, u in PAIRS:
        give(d, u, 1)

    def reduce_step(step, carry):
        for d, u in PAIRS:
            part = partial(d, u, step, mine)
            to_mate(d, u, step).wait_recv()
            to_next(d, u, step - 1).wait_recv()
            acc[d, u, step] += prt[d, u, step] + part
            to_next(d, u, step).start()
        for d, u in PAIRS:
            to_mate(d, u, step - 1).wait_send()
            give(d, u, step + 1)
        return carry

    lax.fori_loop(1, STEPS - 1, reduce_step, 0)
    last = STEPS - 1
    for d, u in PAIRS:
        part = partial(d, u, last, mine)
        to_mate(d, u, last).wait_recv()
        to_next(d, u, last - 1).wait_recv()
        acc[d, u, last] += prt[d, u, last] + part
        src = acc.at[d, u, last]
        gather_next(d, u, 0, src).start()
        gather_mate(d, u, 0, src).start()
        pltpu.make_async_copy(src, spread(d, u, 0), lo_sem.at[d, u]).start()

    def gather_step(t, carry):
        for d, u in PAIRS:
            gather_next(d, u, t - 1, acc.at[d, u, last]).wait_recv()
            gather_next(d, u, t, spread(d, u, t)).start()
            gather_mate(d, u, t, spread(d, u, t)).start()
        return carry

    lax.fori_loop(1, STEPS - 1, gather_step, 0)
    for d, u in PAIRS:
        gather_next(d, u, last - 1, acc.at[d, u, last]).wait_recv()
        gather_mate(d, u, last, spread(d, u, last)).start()

    def drain(t, carry):
        for d, u in PAIRS:
            to_next(d, u, t).wait_send()
            gather_next(d, u, t, acc.at[d, u, last]).wait_send()
            gather_mate(d, u, t, acc.at[d, u, last]).wait()
        return carry

    lax.fori_loop(0, last, drain, 0)
    for d, u in PAIRS:
        gather_mate(d, u, last, acc.at[d, u, last]).wait()
        to_mate(d, u, last - 1).wait_send()
        to_mate(d, u, last).wait_send()
        pltpu.make_async_copy(acc.at[d, u, last], spread(d, u, 0), lo_sem.at[d, u]).wait()


def ring_stage(xt, att, dq, dk, dv, dyp):
    sem = lambda n: pltpu.SemaphoreType.DMA((2, 2, n))
    return pl.pallas_call(
        ring_kernel, name='ring_stage',
        in_specs=[pl.BlockSpec(memory_space=pltpu.VMEM)] * 6,
        out_specs=[pl.BlockSpec(memory_space=pl.ANY)] * 4,
        out_shape=[jax.ShapeDtypeStruct((D, D), F32)] * 4,
        scratch_shapes=[pltpu.VMEM((2, 2, STEPS, 128, 512), F32), pltpu.VMEM((2, 2, STEPS, 128, 512), F32), pltpu.VMEM((2, 2, 2, 128, 512), F32),
                        sem(7), sem(7), sem(8), sem(8), sem(7), sem(7), sem(8), sem(8), pltpu.SemaphoreType.DMA((2, 2))],
        compiler_params=pltpu.CompilerParams(has_side_effects=True, vmem_limit_bytes=56 << 20),
        cost_estimate=pl.CostEstimate(flops=7_000_000_000, bytes_accessed=40_000_000, transcendentals=0),
    )(xt, att, dq, dk, dv, dyp)


def solution(mesh):
    sp_size = mesh.shape['sp']

    def swap(a, bit):
        return lax.ppermute(a, 'sp', [(i, i ^ bit) for i in range(sp_size)])

    def device_step(x, w_q, w_k, w_v, w_o, dy):
        xp, xt, dyp, q, k, v, do, sel = project(x, dy, w_q, w_k, w_v, w_o)
        sel8 = sel[:, 192:288]
        h2 = swap(sel8, 2)
        h1, h3 = swap(sel, 1), swap(h2, 1)
        at, dq, dk, dv, r1, r2, r3 = attention(q, k, v, do, h1, h2, h3)
        r2 = swap(r2 + swap(r3, 1), 2)
        r1 = swap(r1, 1)
        y, att, dxq = out_stage(at, w_o, dq, w_q)
        dx, dkb, dvb = in_stage(dxq, dk, dv, r1, r2, w_k, w_v)
        dw_o, dw_q, dw_k, dw_v = ring_stage(xt, att, dq, dkb, dvb, dyp)
        return y, dx, dw_q, dw_k, dw_v, dw_o

    row_spec = P(('dp', 'sp'), None)
    full_spec = P(None, None)
    grad_spec = P('dp', None)
    return jax.shard_map(device_step, mesh=mesh, in_specs=(row_spec, full_spec, full_spec, full_spec, full_spec, row_spec), out_specs=(row_spec, row_spec, grad_spec, grad_spec, grad_spec, grad_spec), check_vma=False)
```

```python
import jax
import jax.numpy as jnp
from jax import lax
from jax.experimental import pallas as pl
from jax.experimental.pallas import tpu as pltpu
from jax.sharding import PartitionSpec as P


BF = jnp.bfloat16
F32 = jnp.float32
T = 768
D = 1024
CH = 96
NK = 384
LANE = 128
TILE = 256
HALF = 512
SEG = 48
ROWS = 192
HALO = 288
HEAD = 64
MIB = 1 << 20
NT = (((1,), (1,)), ((), ()))


def cost(work):
    return pl.CostEstimate(flops=work * 10**8, bytes_accessed=work * 10**6, transcendentals=0)


def dot(a, b):
    return jnp.dot(a, b, preferred_element_type=F32)


def dot_nt(a, b):
    return lax.dot_general(a, b, NT, preferred_element_type=F32)


def perm_matrix(inverse):
    a = lax.broadcasted_iota(jnp.int32, (LANE, LANE), 1 if inverse else 0)
    b = lax.broadcasted_iota(jnp.int32, (LANE, LANE), 0 if inverse else 1)
    c = a // 16
    res = 4 * (c % 2) + 2 * ((c // 2) % 2) + c // 4
    src = (a % 16) * 8 + res
    return jnp.where(src == b, 1.0, 0.0).astype(BF)


def permute_into(src_ref, dst_ref):
    m = perm_matrix(False)
    for blk in range(T // LANE):
        z = dot(m, src_ref[blk * LANE:(blk + 1) * LANE, :]).astype(BF)
        for c in range(8):
            dst_ref[c * CH + blk * 16:c * CH + blk * 16 + 16, :] = z[c * 16:c * 16 + 16, :]


def unpermute_into(src_ref, dst_ref):
    m = perm_matrix(True)
    for blk in range(T // LANE):
        z = jnp.concatenate([src_ref[c * CH + blk * 16:c * CH + blk * 16 + 16, :] for c in range(8)], axis=0)
        dst_ref[blk * LANE:(blk + 1) * LANE, :] = dot(m, z).astype(BF)


def starts(p):
    return 2 * (p % 2), 2 * (p % 2) + (p // 2) % 2


def left_lanes(n):
    return lax.broadcasted_iota(jnp.int32, (n, LANE), 1) < HEAD


def keys_kernel(x_ref, wk_ref, wv_ref, xp_ref, k_ref, v_ref, sel_ref):
    j = pl.program_id(0)

    @pl.when(j == 0)
    def _():
        permute_into(x_ref, xp_ref)

    k_ref[...] = dot(xp_ref[...], wk_ref[...]).astype(BF)
    v_ref[...] = dot(xp_ref[...], wv_ref[...]).astype(BF)
    for i in range(2):
        s4, s8 = starts(2 * j + i)
        cols = slice(LANE * i, LANE * i + LANE)
        for which, src in enumerate((k_ref, v_ref)):
            for first, n, at in ((s4, ROWS, 0), (s8, CH, ROWS)):
                even = src[pl.ds(pl.multiple_of(first * CH, CH), n), cols]
                odd = src[pl.ds(pl.multiple_of(first * CH + NK, CH), n), cols]
                sel_ref[which, at:at + n, cols] = jnp.where(left_lanes(n), even, odd)


def queries_kernel(xp_ref, dy_ref, wq_ref, wo_ref, xt_ref, dyp_ref, q_ref, do_ref):
    j = pl.program_id(0)

    @pl.when(j == 0)
    def _():
        permute_into(dy_ref, dyp_ref)

    for i in range(2):
        lanes = pl.ds(pl.multiple_of(TILE * j + LANE * i, LANE), LANE)
        xt_ref[LANE * i:LANE * i + LANE, :] = xp_ref[:, lanes].T
    q_ref[...] = (dot(xp_ref[...], wq_ref[...]).astype(BF) * 0.125).astype(BF)
    do_ref[...] = dot_nt(dyp_ref[...], wo_ref[...]).astype(BF)


def project(x, dy, wq, wk, wv, wo):
    full = pl.BlockSpec((T, D), lambda j: (0, 0))
    wcol = pl.BlockSpec((D, TILE), lambda j: (0, j))
    wrow = pl.BlockSpec((TILE, D), lambda j: (j, 0))
    tcol = pl.BlockSpec((T, TILE), lambda j: (0, j))
    tok = jax.ShapeDtypeStruct((T, D), BF)
    price = cost(33)
    xp, k, v, sel = pl.pallas_call(
        keys_kernel, grid=(4,), name='project_keys',
        in_specs=[full, wcol, wcol],
        out_specs=[full, tcol, tcol, pl.BlockSpec((2, HALO, TILE), lambda j: (0, 0, j))],
        out_shape=[tok, tok, tok, jax.ShapeDtypeStruct((2, HALO, D), BF)],
        compiler_params=pltpu.CompilerParams(vmem_limit_bytes=63 * MIB), cost_estimate=price,
    )(x, wk, wv)
    xt, dyp, q, do = pl.pallas_call(
        queries_kernel, grid=(4,), name='project_queries',
        in_specs=[full, full, wcol, wrow],
        out_specs=[pl.BlockSpec((TILE, T), lambda j: (j, 0)), full, tcol, tcol],
        out_shape=[jax.ShapeDtypeStruct((D, T), BF), tok, tok, tok],
        compiler_params=pltpu.CompilerParams(vmem_limit_bytes=63 * MIB), cost_estimate=price,
    )(xp, dy, wq, wo)
    return xt, dyp, q, k, v, do, sel


def attention_kernel(q_ref, k_ref, v_ref, do_ref, h1_ref, h2_ref, h3_ref,
                     at_ref, dq_ref, dk_ref, dv_ref, r1_ref, r2_ref, r3_ref,
                     e_ref, m_ref, acc_ref, dqa_ref, de_ref):
    p = pl.program_id(0)
    s4, s8 = starts(p)
    left = left_lanes(NK)

    def rows_of(ref, first, n):
        return ref[pl.ds(first, n // CH)].reshape(n, ref.shape[-1])

    def pick(ref, b):
        if b < 2:
            return ref[:, b].reshape(NK, LANE)
        first, n = BLOCKS[b]
        return jnp.where(left[:n], rows_of(ref, first, n), rows_of(ref, first + 4, n))

    BLOCKS = {0: (None, NK), 1: (None, NK), 2: (0, NK), 3: (s4, ROWS), 4: (s8, CH)}
    OFFS = (0, NK, T, 1152, 1344)

    def keys(ref, which, b):
        own = pick(ref, b)
        if b < 3:
            return own
        if b == 3:
            return jnp.concatenate([own, h1_ref[which, 0:ROWS, :]], axis=0)
        return jnp.concatenate([own, h1_ref[which, ROWS:HALO, :], h2_ref[which], h3_ref[which]], axis=0)

    def get(ref, e, b):
        w = ref.shape[-1]
        if b < 2:
            return ref[e, :, b].reshape(NK, w)
        first, n = BLOCKS[b]
        return ref[e, pl.ds(first + 4 * e, n // CH)].reshape(n, w)

    def put(ref, e, b, val):
        w = ref.shape[-1]
        if b < 2:
            ref[e, :, b] = val.reshape(8, SEG, w)
        else:
            first, n = BLOCKS[b]
            ref[e, pl.ds(first + 4 * e, n // CH)] = val.reshape(n // CH, 2, SEG, w)

    def head(val, e):
        keep = left[:val.shape[0]] if e == 0 else jnp.logical_not(left[:val.shape[0]])
        return jnp.where(keep, val, jnp.zeros_like(val))

    def wide(val):
        return jnp.concatenate([val, val, val], axis=1)

    for b in range(5):
        n = BLOCKS[b][1]
        qs, ks = pick(q_ref, b), keys(k_ref, 0, b)
        for e in range(2):
            s = dot_nt(head(qs, e), ks)
            e_ref[e, OFFS[b]:OFFS[b] + n, :] = s
            mx = jnp.broadcast_to(jnp.max(s, axis=1, keepdims=True), (n, LANE))
            if b >= 2:
                mx = jnp.maximum(mx, get(m_ref, e, b))
            put(m_ref, e, b, mx)
    ones = jnp.ones((NK, LANE), BF)
    for b in range(5):
        n = BLOCKS[b][1]
        vo = jnp.concatenate([keys(v_ref, 1, b), ones], axis=1)
        for e in range(2):
            ex = jnp.exp(e_ref[e, OFFS[b]:OFFS[b] + n, :] - wide(get(m_ref, e, b)))
            e_ref[e, OFFS[b]:OFFS[b] + n, :] = ex
            o = dot(ex.astype(BF), vo)
            if b >= 2:
                o = o + get(acc_ref, e, b)
            put(acc_ref, e, b, o)
    for c in range(8):
        outs = []
        dd = do_ref[c].reshape(CH, LANE).astype(F32)
        for e in range(2):
            acc = acc_ref[e, c].reshape(CH, TILE)
            linv = 1.0 / acc[:, LANE:]
            o = acc[:, :LANE] * linv
            outs.append(o)
            de = jnp.sum(head(dd * o, e), axis=1, keepdims=True)
            m_ref[e, c] = linv.reshape(2, SEG, LANE)
            de_ref[e, c] = jnp.broadcast_to(de, (CH, LANE)).reshape(2, SEG, LANE)
        at_ref[c] = jnp.where(left[:CH], outs[0], outs[1]).astype(BF).reshape(2, SEG, LANE)
    for b in range(5):
        n = BLOCKS[b][1]
        qs, ks, dos, vs = pick(q_ref, b), keys(k_ref, 0, b), pick(do_ref, b), keys(v_ref, 1, b)
        qt, dot_t = qs.T, dos.T
        dkt, dvt = [], []
        for e in range(2):
            half = slice(HEAD * e, HEAD * e + HEAD)
            pn = e_ref[e, OFFS[b]:OFFS[b] + n, :] * wide(get(m_ref, e, b))
            dp = dot_nt(head(dos, e), vs)
            ds = (pn * (dp - wide(get(de_ref, e, b)))).astype(BF)
            dvt.append(dot(dot_t[half], pn.astype(BF)))
            dkt.append(dot(qt[half], ds))
            dq = dot(ds, ks)
            if b >= 2:
                dq = dq + get(dqa_ref, e, b)
            put(dqa_ref, e, b, dq)
        for which, (parts, own_ref) in enumerate(((dkt, dk_ref), (dvt, dv_ref))):
            g = jnp.concatenate(parts, axis=0).T
            if b < 2:
                own_ref[:, b] = g.reshape(8, SEG, LANE)
                continue
            first = BLOCKS[b][0]
            own = g[:n]
            zero = jnp.zeros_like(own)
            c = n // CH
            shape = (c, 2, SEG, LANE)
            own_ref[pl.ds(first, c)] += jnp.where(left[:n], own, zero).reshape(shape)
            own_ref[pl.ds(first + 4, c)] += jnp.where(left[:n], zero, own).reshape(shape)
            if b == 3:
                r1_ref[which, 0:ROWS, :] = g[ROWS:]
            if b == 4:
                r1_ref[which, ROWS:HALO, :] = g[CH:ROWS]
                r2_ref[which] = g[ROWS:HALO]
                r3_ref[which] = g[HALO:NK]
    for c in range(8):
        pair = jnp.where(left[:CH], dqa_ref[0, c].reshape(CH, LANE), dqa_ref[1, c].reshape(CH, LANE)) * 0.125
        dq_ref[c] = pair.astype(BF).reshape(2, SEG, LANE)


def attention(half, earlier, q, k, v, do, h1, h2, h3):
    row = pl.BlockSpec((8, 2, SEG, LANE), lambda p: (0, 0, 0, p + 4 * half))
    big = pl.BlockSpec((2, HALO, LANE), lambda p: (0, 0, p + 4 * half))
    small = pl.BlockSpec((2, CH, LANE), lambda p: (0, 0, p + 4 * half))
    rbig = pl.BlockSpec((2, HALO, LANE), lambda p: (0, 0, p))
    rsmall = pl.BlockSpec((2, CH, LANE), lambda p: (0, 0, p))
    r = lambda a: a.reshape(8, 2, SEG, D)

    def body(*refs):
        attention_kernel(*refs[:7], *refs[7 + len(earlier):])

    return pl.pallas_call(
        body, grid=(4,), name='attention',
        in_specs=[row] * 4 + [big, small, small] + [pl.BlockSpec(memory_space=pl.ANY)] * len(earlier),
        out_specs=[row] * 4 + [rbig, rsmall, rsmall],
        out_shape=[jax.ShapeDtypeStruct((8, 2, SEG, D), BF)] * 2 + [jax.ShapeDtypeStruct((8, 2, SEG, D), F32)] * 2
        + [jax.ShapeDtypeStruct((2, HALO, D // 2), F32)] + [jax.ShapeDtypeStruct((2, CH, D // 2), F32)] * 2,
        scratch_shapes=[pltpu.VMEM((2, 1440, NK), F32), pltpu.VMEM((2, 8, 2, SEG, LANE), F32), pltpu.VMEM((2, 8, 2, SEG, TILE), F32),
                        pltpu.VMEM((2, 8, 2, SEG, LANE), F32), pltpu.VMEM((2, 8, 2, SEG, LANE), F32)],
        input_output_aliases={7 + n: n for n in range(len(earlier))},
        compiler_params=pltpu.CompilerParams(vmem_limit_bytes=63 * MIB),
       cost_estimate=cost(150),
    )(r(q), r(k), r(v), r(do), h1, h2, h3, *earlier)


def out_kernel(at_ref, wo_ref, y_ref, att_ref, yp_ref):
    j = pl.program_id(0)
    yp_ref[...] = dot(at_ref[...], wo_ref[...]).astype(BF)
    unpermute_into(yp_ref, y_ref)

    @pl.when(j == 0)
    def _():
        for i in range(8):
            att_ref[LANE * i:LANE * i + LANE, :] = at_ref[:, LANE * i:LANE * i + LANE].T


def out_stage(at, wo):
    full = pl.BlockSpec((T, D), lambda j: (0, 0))
    col = pl.BlockSpec((D, TILE), lambda j: (0, j))
    tcol = pl.BlockSpec((T, TILE), lambda j: (0, j))
    return pl.pallas_call(
        out_kernel, grid=(4,), name='out_stage',
        in_specs=[full, col],
        out_specs=[tcol, pl.BlockSpec((D, T), lambda j: (0, 0))],
        out_shape=[jax.ShapeDtypeStruct((T, D), BF), jax.ShapeDtypeStruct((D, T), BF)],
        scratch_shapes=[pltpu.VMEM((T, TILE), BF)],
        compiler_params=pltpu.CompilerParams(vmem_limit_bytes=63 * MIB),
       cost_estimate=cost(17),
    )(at, wo)


def in_kernel(dk_ref, dv_ref, r1a_ref, r1b_ref, r2a_ref, r2b_ref, dkb_ref, dvb_ref, sum_ref):
    j = pl.program_id(0)
    for which, (own_ref, g_ref) in enumerate(((dk_ref, dkb_ref), (dv_ref, dvb_ref))):
        sum_ref[...] = own_ref[...]
        for i in range(2):
            s4, s8 = starts(2 * j + i)
            cols = slice(LANE * i, LANE * i + LANE)
            one = jnp.where(j < 2, r1a_ref[which, :, cols], r1b_ref[which, :, cols])
            a4 = one[:ROWS]
            a8 = one[ROWS:] + jnp.where(j < 2, r2a_ref[which, :, cols], r2b_ref[which, :, cols])
            for first, n, add in ((s4, ROWS, a4), (s8, CH, a8)):
                keep = left_lanes(n)
                zero = jnp.zeros_like(add)
                sum_ref[pl.ds(pl.multiple_of(first * CH, CH), n), cols] += jnp.where(keep, add, zero)
                sum_ref[pl.ds(pl.multiple_of(first * CH + NK, CH), n), cols] += jnp.where(keep, zero, add)
        g_ref[...] = sum_ref[...].astype(BF)


def in_stage(dk, dv, r1a, r1b, r2a, r2b):
    tcol = pl.BlockSpec((T, TILE), lambda j: (0, j))
    first = lambda n: pl.BlockSpec((2, n, TILE), lambda j: (0, 0, jnp.minimum(j, 1)))
    second = lambda n: pl.BlockSpec((2, n, TILE), lambda j: (0, 0, jnp.maximum(j - 2, 0)))
    return pl.pallas_call(
        in_kernel, grid=(4,), name='in_stage',
        in_specs=[tcol, tcol, first(HALO), second(HALO), first(CH), second(CH)],
        out_specs=[tcol, tcol],
        out_shape=[jax.ShapeDtypeStruct((T, D), BF)] * 2,
        scratch_shapes=[pltpu.VMEM((T, TILE), F32)],
        compiler_params=pltpu.CompilerParams(vmem_limit_bytes=63 * MIB),
       cost_estimate=cost(1),
    )(dk, dv, r1a, r1b, r2a, r2b)


STEPS = 8
PAIRS = tuple((d, u) for u in range(2) for d in range(2))


def ring_kernel(xt_ref, att_ref, dq_ref, dk_ref, dv_ref, dy_ref, wq_hbm, wk_hbm, wv_hbm, *refs):
    outs, dx_ref = refs[:4], refs[4]
    acc, prt, stage, wq_ref, wk_ref, wv_ref, dxp_ref, rs_send, rs_recv, pt_send, pt_recv, ag_send, ag_recv, cc_send, cc_recv, lo_sem, ld_sem = refs[5:]
    loads = [pltpu.make_async_copy(a, b, ld_sem.at[n]) for n, (a, b) in enumerate(((wq_hbm, wq_ref), (wk_hbm, wk_ref), (wv_hbm, wv_ref)))]
    for load in loads:
        load.start()
    out = ((outs[0], outs[1]), (outs[2], outs[3]))
    lhs = ((att_ref, xt_ref), (xt_ref, xt_ref))
    rhs = ((dy_ref, dq_ref), (dk_ref, dv_ref))
    s = lax.axis_index('sp')
    core, y, z = s % 2, (s // 2) % 2, s // 4
    pos = z + y * (7 - 2 * z)
    mate = {'sp': s + 1 - 2 * core}

    def member(r):
        r = r % STEPS
        row = r // 4
        return {'sp': (r + row * (7 - 2 * r)) * 4 + row * 2 + core}

    ahead = (member(pos + 1), member(pos + STEPS - 1))
    mine = pl.ds(pl.multiple_of(HALF * core, HALF), HALF)
    other = pl.ds(pl.multiple_of(HALF * (1 - core), HALF), HALF)

    def shard(d, step):
        return (pos + 15 - step) % STEPS if d == 0 else (pos + 1 + step) % STEPS

    def rows(i):
        return pl.ds(pl.multiple_of(LANE * i, LANE), LANE)

    def partial(d, u, step, cols):
        return dot(lhs[d][u][rows(shard(d, step)), :], rhs[d][u][:, cols])

    def remote(src, dst, send, recv, peer):
        return pltpu.make_async_remote_copy(src_ref=src, dst_ref=dst, send_sem=send, recv_sem=recv, device_id=peer, device_id_type=pl.DeviceIdType.MESH)

    def to_mate(d, u, step):
        return remote(stage.at[d, u, step % 2], prt.at[d, u, step], pt_send.at[d, u, step], pt_recv.at[d, u, step], mate)

    def to_next(d, u, step):
        return remote(acc.at[d, u, step], acc.at[d, u, step + 1], rs_send.at[d, u, step], rs_recv.at[d, u, step], ahead[d])

    def give(d, u, step):
        stage[d, u, step % 2] = partial(d, u, step, other)
        to_mate(d, u, step).start()

    def spread(d, u, t):
        i = (pos + 8 - t) % STEPS if d == 0 else (pos + t) % STEPS
        return out[d][u].at[rows(i), mine]

    def gather_next(d, u, t, src):
        return remote(src, spread(d, u, t), ag_send.at[d, u, t], ag_recv.at[d, u, t], ahead[d])

    def gather_mate(d, u, t, src):
        return remote(src, spread(d, u, t), cc_send.at[d, u, t], cc_recv.at[d, u, t], mate)

    for d, u in PAIRS:
        give(d, u, 0)
    for d, u in PAIRS:
        acc[d, u, 0] = partial(d, u, 0, mine)
        to_mate(d, u, 0).wait_recv()
        acc[d, u, 0] += prt[d, u, 0]
        to_next(d, u, 0).start()
    for d, u in PAIRS:
        give(d, u, 1)

    def reduce_step(step, carry):
        for d, u in PAIRS:
            part = partial(d, u, step, mine)
            to_mate(d, u, step).wait_recv()
            to_next(d, u, step - 1).wait_recv()
            acc[d, u, step] += prt[d, u, step] + part
            to_next(d, u, step).start()
        for d, u in PAIRS:
            to_mate(d, u, step - 1).wait_send()
            give(d, u, step + 1)
        return carry

    lax.fori_loop(1, STEPS - 1, reduce_step, 0)
    last = STEPS - 1
    for d, u in PAIRS:
        part = partial(d, u, last, mine)
        to_mate(d, u, last).wait_recv()
        to_next(d, u, last - 1).wait_recv()
        acc[d, u, last] += prt[d, u, last] + part
        src = acc.at[d, u, last]
        gather_next(d, u, 0, src).start()
        gather_mate(d, u, 0, src).start()
        pltpu.make_async_copy(src, spread(d, u, 0), lo_sem.at[d, u]).start()

    for load in loads:
        load.wait()

    def gather_step(t, carry):
        for d, u in PAIRS:
            gather_next(d, u, t - 1, acc.at[d, u, last]).wait_recv()
            gather_next(d, u, t, spread(d, u, t)).start()
            gather_mate(d, u, t, spread(d, u, t)).start()
        block = pl.ds(pl.multiple_of(LANE * (t - 1), LANE), LANE)
        total = dot_nt(dq_ref[block, :], wq_ref[...]) + dot_nt(dk_ref[block, :], wk_ref[...]) + dot_nt(dv_ref[block, :], wv_ref[...])
        dxp_ref[block, :] = total.astype(BF)
        return carry

    lax.fori_loop(1, STEPS - 1, gather_step, 0)
    for d, u in PAIRS:
        gather_next(d, u, last - 1, acc.at[d, u, last]).wait_recv()
        gather_mate(d, u, last, spread(d, u, last)).start()

    unpermute_into(dxp_ref, dx_ref)

    def drain(t, carry):
        for d, u in PAIRS:
            to_next(d, u, t).wait_send()
            gather_next(d, u, t, acc.at[d, u, last]).wait_send()
            gather_mate(d, u, t, acc.at[d, u, last]).wait()
        return carry

    lax.fori_loop(0, last, drain, 0)
    for d, u in PAIRS:
        gather_mate(d, u, last, acc.at[d, u, last]).wait()
        to_mate(d, u, last - 1).wait_send()
        to_mate(d, u, last).wait_send()
        pltpu.make_async_copy(acc.at[d, u, last], spread(d, u, 0), lo_sem.at[d, u]).wait()


def ring_stage(xt, att, dq, dk, dv, dyp, wq, wk, wv):
    sem = lambda n: pltpu.SemaphoreType.DMA((2, 2, n))
    return pl.pallas_call(
        ring_kernel, name='ring_stage',
        in_specs=[pl.BlockSpec(memory_space=pltpu.VMEM)] * 6 + [pl.BlockSpec(memory_space=pl.ANY)] * 3,
        out_specs=[pl.BlockSpec(memory_space=pl.ANY)] * 4 + [pl.BlockSpec(memory_space=pltpu.VMEM)],
        out_shape=[jax.ShapeDtypeStruct((D, D), F32)] * 4 + [jax.ShapeDtypeStruct((T, D), BF)],
        scratch_shapes=[pltpu.VMEM((2, 2, STEPS, LANE, HALF), F32), pltpu.VMEM((2, 2, STEPS, LANE, HALF), F32), pltpu.VMEM((2, 2, 2, LANE, HALF), F32),
                        pltpu.VMEM((D, D), BF), pltpu.VMEM((D, D), BF), pltpu.VMEM((D, D), BF), pltpu.VMEM((T, D), BF),
                        sem(7), sem(7), sem(8), sem(8), sem(7), sem(7), sem(8), sem(8), pltpu.SemaphoreType.DMA((2, 2)), pltpu.SemaphoreType.DMA((3,))],
        compiler_params=pltpu.CompilerParams(has_side_effects=True, vmem_limit_bytes=63 * MIB),
       cost_estimate=cost(110),
    )(xt, att, dq, dk, dv, dyp, wq, wk, wv)


def solution(mesh):
    sp_size = mesh.shape['sp']

    def swap(a, bit):
        return lax.ppermute(a, 'sp', [(i, i ^ bit) for i in range(sp_size)])

    def device_work(x, w_q, w_k, w_v, w_o, dy):
        xt, dyp, q, k, v, do, sel = project(x, dy, w_q, w_k, w_v, w_o)
        sel8 = sel[:, ROWS:HALO]
        h2 = swap(sel8, 2)
        h1 = swap(sel, 1)
        h2, q = lax.optimization_barrier((h2, q))
        h3 = swap(h2, 1)
        grads, r1, r2 = (), [], []
        for half in range(2):
            *grads, one, two, three = attention(half, tuple(grads), q, k, v, do, h1, h2, h3)
            two = two + swap(three, 1)
            one, two, grads[0] = lax.optimization_barrier((one, two, grads[0]))
            r2.append(swap(two, 2))
            r1.append(swap(one, 1))
        at, dq, dk, dv = (g.reshape(T, D) for g in grads)
        y, att = out_stage(at, w_o)
        dkb, dvb = in_stage(dk, dv, *r1, *r2)
        dw_o, dw_q, dw_k, dw_v, dx = ring_stage(xt, att, dq, dkb, dvb, dyp, w_q, w_k, w_v)
        return y, dx, dw_q, dw_k, dw_v, dw_o

    row_spec = P(('dp', 'sp'), None)
    full_spec = P(None, None)
    grad_spec = P('dp', None)
    return jax.shard_map(device_work, mesh=mesh, in_specs=(row_spec, full_spec, full_spec, full_spec, full_spec, row_spec), out_specs=(row_spec, row_spec, grad_spec, grad_spec, grad_spec, grad_spec), check_vma=False)
```

```python
import jax
import jax.numpy as jnp
from jax import lax
from jax.experimental import pallas as pl
from jax.experimental.pallas import tpu as pltpu
from jax.sharding import PartitionSpec as P


BF = jnp.bfloat16
F32 = jnp.float32
T = 768
D = 1024
CH = 96
NK = 384
LANE = 128
TILE = 256
HALF = 512
SEG = 48
ROWS = 192
HALO = 288
HEAD = 64
MIB = 1 << 20
NT = (((1,), (1,)), ((), ()))


def cost(work):
    return pl.CostEstimate(flops=work * 10**8, bytes_accessed=work * 10**6, transcendentals=0)


def dot(a, b):
    return jnp.dot(a, b, preferred_element_type=F32)


def dot_nt(a, b):
    return lax.dot_general(a, b, NT, preferred_element_type=F32)


def perm_matrix(inverse):
    a = lax.broadcasted_iota(jnp.int32, (LANE, LANE), 1 if inverse else 0)
    b = lax.broadcasted_iota(jnp.int32, (LANE, LANE), 0 if inverse else 1)
    c = a // 16
    res = 4 * (c % 2) + 2 * ((c // 2) % 2) + c // 4
    src = (a % 16) * 8 + res
    return jnp.where(src == b, 1.0, 0.0).astype(BF)


def permute_into(src_ref, dst_ref):
    m = perm_matrix(False)
    for blk in range(T // LANE):
        z = dot(m, src_ref[blk * LANE:(blk + 1) * LANE, :]).astype(BF)
        for c in range(8):
            dst_ref[c * CH + blk * 16:c * CH + blk * 16 + 16, :] = z[c * 16:c * 16 + 16, :]


def unpermute_into(src_ref, dst_ref):
    m = perm_matrix(True)
    for blk in range(T // LANE):
        z = jnp.concatenate([src_ref[c * CH + blk * 16:c * CH + blk * 16 + 16, :] for c in range(8)], axis=0)
        dst_ref[blk * LANE:(blk + 1) * LANE, :] = dot(m, z).astype(BF)


def starts(p):
    return 2 * (p % 2), 2 * (p % 2) + (p // 2) % 2


def left_lanes(n):
    return lax.broadcasted_iota(jnp.int32, (n, LANE), 1) < HEAD


def keys_kernel(x_ref, wk_ref, wv_ref, xp_ref, k_ref, v_ref, sel_ref):
    j = pl.program_id(0)

    @pl.when(j == 0)
    def _():
        permute_into(x_ref, xp_ref)

    k_ref[...] = dot(xp_ref[...], wk_ref[...]).astype(BF)
    v_ref[...] = dot(xp_ref[...], wv_ref[...]).astype(BF)
    for i in range(2):
        s4, s8 = starts(2 * j + i)
        cols = slice(LANE * i, LANE * i + LANE)
        for which, src in enumerate((k_ref, v_ref)):
            for first, n, at in ((s4, ROWS, 0), (s8, CH, ROWS)):
                even = src[pl.ds(pl.multiple_of(first * CH, CH), n), cols]
                odd = src[pl.ds(pl.multiple_of(first * CH + NK, CH), n), cols]
                sel_ref[which, at:at + n, cols] = jnp.where(left_lanes(n), even, odd)


def queries_kernel(xp_ref, dy_ref, wq_ref, wo_ref, xt_ref, dyp_ref, q_ref, do_ref):
    j = pl.program_id(0)

    @pl.when(j == 0)
    def _():
        permute_into(dy_ref, dyp_ref)

    for i in range(2):
        lanes = pl.ds(pl.multiple_of(TILE * j + LANE * i, LANE), LANE)
        xt_ref[LANE * i:LANE * i + LANE, :] = xp_ref[:, lanes].T
    q_ref[...] = (dot(xp_ref[...], wq_ref[...]).astype(BF) * 0.125).astype(BF)
    do_ref[...] = dot_nt(dyp_ref[...], wo_ref[...]).astype(BF)


def project(x, dy, wq, wk, wv, wo):
    full = pl.BlockSpec((T, D), lambda j: (0, 0))
    wcol = pl.BlockSpec((D, TILE), lambda j: (0, j))
    wrow = pl.BlockSpec((TILE, D), lambda j: (j, 0))
    tcol = pl.BlockSpec((T, TILE), lambda j: (0, j))
    tok = jax.ShapeDtypeStruct((T, D), BF)
    price = cost(33)
    xp, k, v, sel = pl.pallas_call(
        keys_kernel, grid=(4,), name='project_keys',
        in_specs=[full, wcol, wcol],
        out_specs=[full, tcol, tcol, pl.BlockSpec((2, HALO, TILE), lambda j: (0, 0, j))],
        out_shape=[tok, tok, tok, jax.ShapeDtypeStruct((2, HALO, D), BF)],
        compiler_params=pltpu.CompilerParams(vmem_limit_bytes=63 * MIB), cost_estimate=price,
    )(x, wk, wv)
    xt, dyp, q, do = pl.pallas_call(
        queries_kernel, grid=(4,), name='project_queries',
        in_specs=[full, full, wcol, wrow],
        out_specs=[pl.BlockSpec((TILE, T), lambda j: (j, 0)), full, tcol, tcol],
        out_shape=[jax.ShapeDtypeStruct((D, T), BF), tok, tok, tok],
        compiler_params=pltpu.CompilerParams(vmem_limit_bytes=63 * MIB), cost_estimate=price,
    )(xp, dy, wq, wo)
    return xt, dyp, q, k, v, do, sel


def attention_kernel(q_ref, k_ref, v_ref, do_ref, h1_ref, h2_ref, h3_ref,
                     at_ref, dq_ref, dk_ref, dv_ref, r1_ref, r2_ref, r3_ref,
                     e_ref, m_ref, acc_ref, dqa_ref, de_ref):
    p = pl.program_id(0)
    s4, s8 = starts(p)
    left = left_lanes(NK)

    def rows_of(ref, first, n):
        return ref[pl.ds(first, n // CH)].reshape(n, ref.shape[-1])

    def pick(ref, b):
        if b < 2:
            return ref[:, b].reshape(NK, LANE)
        first, n = BLOCKS[b]
        return jnp.where(left[:n], rows_of(ref, first, n), rows_of(ref, first + 4, n))

    BLOCKS = {0: (None, NK), 1: (None, NK), 2: (0, NK), 3: (s4, ROWS), 4: (s8, CH)}
    OFFS = (0, NK, T, 1152, 1344)

    def keys(ref, which, b):
        own = pick(ref, b)
        if b < 3:
            return own
        if b == 3:
            return jnp.concatenate([own, h1_ref[which, 0:ROWS, :]], axis=0)
        return jnp.concatenate([own, h1_ref[which, ROWS:HALO, :], h2_ref[which], h3_ref[which]], axis=0)

    def get(ref, e, b):
        w = ref.shape[-1]
        if b < 2:
            return ref[e, :, b].reshape(NK, w)
        first, n = BLOCKS[b]
        return ref[e, pl.ds(first + 4 * e, n // CH)].reshape(n, w)

    def put(ref, e, b, val):
        w = ref.shape[-1]
        if b < 2:
            ref[e, :, b] = val.reshape(8, SEG, w)
        else:
            first, n = BLOCKS[b]
            ref[e, pl.ds(first + 4 * e, n // CH)] = val.reshape(n // CH, 2, SEG, w)

    def head(val, e):
        keep = left[:val.shape[0]] if e == 0 else jnp.logical_not(left[:val.shape[0]])
        return jnp.where(keep, val, jnp.zeros_like(val))

    def wide(val):
        return jnp.concatenate([val, val, val], axis=1)

    for b in range(5):
        n = BLOCKS[b][1]
        qs, ks = pick(q_ref, b), keys(k_ref, 0, b)
        for e in range(2):
            s = dot_nt(head(qs, e), ks)
            e_ref[e, OFFS[b]:OFFS[b] + n, :] = s
            mx = jnp.broadcast_to(jnp.max(s, axis=1, keepdims=True), (n, LANE))
            if b >= 2:
                mx = jnp.maximum(mx, get(m_ref, e, b))
            put(m_ref, e, b, mx)
    ones = jnp.ones((NK, LANE), BF)
    for b in range(5):
        n = BLOCKS[b][1]
        vo = jnp.concatenate([keys(v_ref, 1, b), ones], axis=1)
        for e in range(2):
            ex = jnp.exp(e_ref[e, OFFS[b]:OFFS[b] + n, :] - wide(get(m_ref, e, b)))
            e_ref[e, OFFS[b]:OFFS[b] + n, :] = ex
            o = dot(ex.astype(BF), vo)
            if b >= 2:
                o = o + get(acc_ref, e, b)
            put(acc_ref, e, b, o)
    for c in range(8):
        outs = []
        dd = do_ref[c].reshape(CH, LANE).astype(F32)
        for e in range(2):
            acc = acc_ref[e, c].reshape(CH, TILE)
            linv = 1.0 / acc[:, LANE:]
            o = acc[:, :LANE] * linv
            outs.append(o)
            de = jnp.sum(head(dd * o, e), axis=1, keepdims=True)
            m_ref[e, c] = linv.reshape(2, SEG, LANE)
            de_ref[e, c] = jnp.broadcast_to(de, (CH, LANE)).reshape(2, SEG, LANE)
        at_ref[c] = jnp.where(left[:CH], outs[0], outs[1]).astype(BF).reshape(2, SEG, LANE)
    for b in range(5):
        n = BLOCKS[b][1]
        qs, ks, dos, vs = pick(q_ref, b), keys(k_ref, 0, b), pick(do_ref, b), keys(v_ref, 1, b)
        qt, dot_t = qs.T, dos.T
        dkt, dvt = [], []
        for e in range(2):
            half = slice(HEAD * e, HEAD * e + HEAD)
            pn = e_ref[e, OFFS[b]:OFFS[b] + n, :] * wide(get(m_ref, e, b))
            dp = dot_nt(head(dos, e), vs)
            ds = (pn * (dp - wide(get(de_ref, e, b)))).astype(BF)
            dvt.append(dot(dot_t[half], pn.astype(BF)))
            dkt.append(dot(qt[half], ds))
            dq = dot(ds, ks)
            if b >= 2:
                dq = dq + get(dqa_ref, e, b)
            put(dqa_ref, e, b, dq)
        for which, (parts, own_ref) in enumerate(((dkt, dk_ref), (dvt, dv_ref))):
            g = jnp.concatenate(parts, axis=0).T
            if b < 2:
                own_ref[:, b] = g.reshape(8, SEG, LANE)
                continue
            first = BLOCKS[b][0]
            own = g[:n]
            zero = jnp.zeros_like(own)
            c = n // CH
            shape = (c, 2, SEG, LANE)
            own_ref[pl.ds(first, c)] += jnp.where(left[:n], own, zero).reshape(shape)
            own_ref[pl.ds(first + 4, c)] += jnp.where(left[:n], zero, own).reshape(shape)
            if b == 3:
                r1_ref[which, 0:ROWS, :] = g[ROWS:]
            if b == 4:
                r1_ref[which, ROWS:HALO, :] = g[CH:ROWS]
                r2_ref[which] = g[ROWS:HALO]
                r3_ref[which] = g[HALO:NK]
    for c in range(8):
        pair = jnp.where(left[:CH], dqa_ref[0, c].reshape(CH, LANE), dqa_ref[1, c].reshape(CH, LANE)) * 0.125
        dq_ref[c] = pair.astype(BF).reshape(2, SEG, LANE)


def attention(half, earlier, q, k, v, do, h1, h2, h3):
    row = pl.BlockSpec((8, 2, SEG, LANE), lambda p: (0, 0, 0, p + 4 * half))
    big = pl.BlockSpec((2, HALO, LANE), lambda p: (0, 0, p + 4 * half))
    small = pl.BlockSpec((2, CH, LANE), lambda p: (0, 0, p + 4 * half))
    rbig = pl.BlockSpec((2, HALO, LANE), lambda p: (0, 0, p))
    rsmall = pl.BlockSpec((2, CH, LANE), lambda p: (0, 0, p))
    r = lambda a: a.reshape(8, 2, SEG, D)

    def body(*refs):
        attention_kernel(*refs[:7], *refs[7 + len(earlier):])

    return pl.pallas_call(
        body, grid=(4,), name='attention',
        in_specs=[row] * 4 + [big, small, small] + [pl.BlockSpec(memory_space=pl.ANY)] * len(earlier),
        out_specs=[row] * 4 + [rbig, rsmall, rsmall],
        out_shape=[jax.ShapeDtypeStruct((8, 2, SEG, D), BF)] * 2 + [jax.ShapeDtypeStruct((8, 2, SEG, D), F32)] * 2
        + [jax.ShapeDtypeStruct((2, HALO, D // 2), F32)] + [jax.ShapeDtypeStruct((2, CH, D // 2), F32)] * 2,
        scratch_shapes=[pltpu.VMEM((2, 1440, NK), F32), pltpu.VMEM((2, 8, 2, SEG, LANE), F32), pltpu.VMEM((2, 8, 2, SEG, TILE), F32),
                        pltpu.VMEM((2, 8, 2, SEG, LANE), F32), pltpu.VMEM((2, 8, 2, SEG, LANE), F32)],
        input_output_aliases={7 + n: n for n in range(len(earlier))},
        compiler_params=pltpu.CompilerParams(vmem_limit_bytes=63 * MIB),
       cost_estimate=cost(150),
    )(r(q), r(k), r(v), r(do), h1, h2, h3, *earlier)


def out_kernel(at_ref, wo_ref, y_ref, att_ref, yp_ref):
    j = pl.program_id(0)
    yp_ref[...] = dot(at_ref[...], wo_ref[...]).astype(BF)
    unpermute_into(yp_ref, y_ref)

    @pl.when(j == 0)
    def _():
        for i in range(8):
            att_ref[LANE * i:LANE * i + LANE, :] = at_ref[:, LANE * i:LANE * i + LANE].T


def out_stage(at, wo):
    full = pl.BlockSpec((T, D), lambda j: (0, 0))
    col = pl.BlockSpec((D, TILE), lambda j: (0, j))
    tcol = pl.BlockSpec((T, TILE), lambda j: (0, j))
    return pl.pallas_call(
        out_kernel, grid=(4,), name='out_stage',
        in_specs=[full, col],
        out_specs=[tcol, pl.BlockSpec((D, T), lambda j: (0, 0))],
        out_shape=[jax.ShapeDtypeStruct((T, D), BF), jax.ShapeDtypeStruct((D, T), BF)],
        scratch_shapes=[pltpu.VMEM((T, TILE), BF)],
        compiler_params=pltpu.CompilerParams(vmem_limit_bytes=63 * MIB),
       cost_estimate=cost(17),
    )(at, wo)


def in_kernel(dk_ref, dv_ref, r1a_ref, r1b_ref, r2a_ref, r2b_ref, dkb_ref, dvb_ref, sum_ref):
    j = pl.program_id(0)
    for which, (own_ref, g_ref) in enumerate(((dk_ref, dkb_ref), (dv_ref, dvb_ref))):
        sum_ref[...] = own_ref[...]
        for i in range(2):
            s4, s8 = starts(2 * j + i)
            cols = slice(LANE * i, LANE * i + LANE)
            one = jnp.where(j < 2, r1a_ref[which, :, cols], r1b_ref[which, :, cols])
            a4 = one[:ROWS]
            a8 = one[ROWS:] + jnp.where(j < 2, r2a_ref[which, :, cols], r2b_ref[which, :, cols])
            for first, n, add in ((s4, ROWS, a4), (s8, CH, a8)):
                keep = left_lanes(n)
                zero = jnp.zeros_like(add)
                sum_ref[pl.ds(pl.multiple_of(first * CH, CH), n), cols] += jnp.where(keep, add, zero)
                sum_ref[pl.ds(pl.multiple_of(first * CH + NK, CH), n), cols] += jnp.where(keep, zero, add)
        g_ref[...] = sum_ref[...].astype(BF)


def in_stage(dk, dv, r1a, r1b, r2a, r2b):
    tcol = pl.BlockSpec((T, TILE), lambda j: (0, j))
    first = lambda n: pl.BlockSpec((2, n, TILE), lambda j: (0, 0, jnp.minimum(j, 1)))
    second = lambda n: pl.BlockSpec((2, n, TILE), lambda j: (0, 0, jnp.maximum(j - 2, 0)))
    return pl.pallas_call(
        in_kernel, grid=(4,), name='in_stage',
        in_specs=[tcol, tcol, first(HALO), second(HALO), first(CH), second(CH)],
        out_specs=[tcol, tcol],
        out_shape=[jax.ShapeDtypeStruct((T, D), BF)] * 2,
        scratch_shapes=[pltpu.VMEM((T, TILE), F32)],
        compiler_params=pltpu.CompilerParams(vmem_limit_bytes=63 * MIB),
       cost_estimate=cost(1),
    )(dk, dv, r1a, r1b, r2a, r2b)


STEPS = 8
PAIRS = tuple((d, u) for u in range(2) for d in range(2))


def ring_kernel(xt_ref, att_ref, dq_ref, dk_ref, dv_ref, dy_ref, wq_hbm, wk_hbm, wv_hbm, *refs):
    outs, dxp_ref = refs[:4], refs[4]
    acc, prt, stage, wq_ref, wk_ref, wv_ref, rs_send, rs_recv, pt_send, pt_recv, ag_send, ag_recv, cc_send, cc_recv, lo_sem, ld_sem = refs[5:]
    loads = [pltpu.make_async_copy(a, b, ld_sem.at[n]) for n, (a, b) in enumerate(((wq_hbm, wq_ref), (wk_hbm, wk_ref), (wv_hbm, wv_ref)))]
    for load in loads:
        load.start()
    out = ((outs[0], outs[1]), (outs[2], outs[3]))
    lhs = ((att_ref, xt_ref), (xt_ref, xt_ref))
    rhs = ((dy_ref, dq_ref), (dk_ref, dv_ref))
    s = lax.axis_index('sp')
    core, y, z = s % 2, (s // 2) % 2, s // 4
    pos = z + y * (7 - 2 * z)
    mate = {'sp': s + 1 - 2 * core}

    def member(r):
        r = r % STEPS
        row = r // 4
        return {'sp': (r + row * (7 - 2 * r)) * 4 + row * 2 + core}

    ahead = (member(pos + 1), member(pos + STEPS - 1))
    mine = pl.ds(pl.multiple_of(HALF * core, HALF), HALF)
    other = pl.ds(pl.multiple_of(HALF * (1 - core), HALF), HALF)

    def shard(d, step):
        return (pos + 15 - step) % STEPS if d == 0 else (pos + 1 + step) % STEPS

    def rows(i):
        return pl.ds(pl.multiple_of(LANE * i, LANE), LANE)

    def partial(d, u, step, cols):
        return dot(lhs[d][u][rows(shard(d, step)), :], rhs[d][u][:, cols])

    def remote(src, dst, send, recv, peer):
        return pltpu.make_async_remote_copy(src_ref=src, dst_ref=dst, send_sem=send, recv_sem=recv, device_id=peer, device_id_type=pl.DeviceIdType.MESH)

    def to_mate(d, u, step):
        return remote(stage.at[d, u, step % 2], prt.at[d, u, step], pt_send.at[d, u, step], pt_recv.at[d, u, step], mate)

    def to_next(d, u, step):
        return remote(acc.at[d, u, step], acc.at[d, u, step + 1], rs_send.at[d, u, step], rs_recv.at[d, u, step], ahead[d])

    def give(d, u, step):
        stage[d, u, step % 2] = partial(d, u, step, other)
        to_mate(d, u, step).start()

    def spread(d, u, t):
        i = (pos + 8 - t) % STEPS if d == 0 else (pos + t) % STEPS
        return out[d][u].at[rows(i), mine]

    def gather_next(d, u, t, src):
        return remote(src, spread(d, u, t), ag_send.at[d, u, t], ag_recv.at[d, u, t], ahead[d])

    def gather_mate(d, u, t, src):
        return remote(src, spread(d, u, t), cc_send.at[d, u, t], cc_recv.at[d, u, t], mate)

    for d, u in PAIRS:
        give(d, u, 0)
    for d, u in PAIRS:
        acc[d, u, 0] = partial(d, u, 0, mine)
        to_mate(d, u, 0).wait_recv()
        acc[d, u, 0] += prt[d, u, 0]
        to_next(d, u, 0).start()
    for d, u in PAIRS:
        give(d, u, 1)

    def reduce_step(step, carry):
        for d, u in PAIRS:
            part = partial(d, u, step, mine)
            to_mate(d, u, step).wait_recv()
            to_next(d, u, step - 1).wait_recv()
            acc[d, u, step] += prt[d, u, step] + part
            to_next(d, u, step).start()
        for d, u in PAIRS:
            to_mate(d, u, step - 1).wait_send()
            give(d, u, step + 1)
        return carry

    lax.fori_loop(1, STEPS - 1, reduce_step, 0)
    last = STEPS - 1
    for d, u in PAIRS:
        part = partial(d, u, last, mine)
        to_mate(d, u, last).wait_recv()
        to_next(d, u, last - 1).wait_recv()
        acc[d, u, last] += prt[d, u, last] + part
        src = acc.at[d, u, last]
        gather_next(d, u, 0, src).start()
        gather_mate(d, u, 0, src).start()
        pltpu.make_async_copy(src, spread(d, u, 0), lo_sem.at[d, u]).start()

    for load in loads:
        load.wait()

    def gather_step(t, carry):
        for d, u in PAIRS:
            gather_next(d, u, t - 1, acc.at[d, u, last]).wait_recv()
            gather_next(d, u, t, spread(d, u, t)).start()
            gather_mate(d, u, t, spread(d, u, t)).start()
        block = pl.ds(pl.multiple_of(LANE * (t - 1), LANE), LANE)
        total = dot_nt(dq_ref[block, :], wq_ref[...]) + dot_nt(dk_ref[block, :], wk_ref[...]) + dot_nt(dv_ref[block, :], wv_ref[...])
        dxp_ref[block, :] = total.astype(BF)
        return carry

    lax.fori_loop(1, STEPS - 1, gather_step, 0)
    for d, u in PAIRS:
        gather_next(d, u, last - 1, acc.at[d, u, last]).wait_recv()
        gather_mate(d, u, last, spread(d, u, last)).start()

    def drain(t, carry):
        for d, u in PAIRS:
            to_next(d, u, t).wait_send()
            gather_next(d, u, t, acc.at[d, u, last]).wait_send()
            gather_mate(d, u, t, acc.at[d, u, last]).wait()
        return carry

    lax.fori_loop(0, last, drain, 0)
    for d, u in PAIRS:
        gather_mate(d, u, last, acc.at[d, u, last]).wait()
        to_mate(d, u, last - 1).wait_send()
        to_mate(d, u, last).wait_send()
        pltpu.make_async_copy(acc.at[d, u, last], spread(d, u, 0), lo_sem.at[d, u]).wait()


def ring_stage(xt, att, dq, dk, dv, dyp, wq, wk, wv):
    sem = lambda n: pltpu.SemaphoreType.DMA((2, 2, n))
    return pl.pallas_call(
        ring_kernel, name='ring_stage',
        in_specs=[pl.BlockSpec(memory_space=pltpu.VMEM)] * 6 + [pl.BlockSpec(memory_space=pl.ANY)] * 3,
        out_specs=[pl.BlockSpec(memory_space=pl.ANY)] * 4 + [pl.BlockSpec(memory_space=pltpu.VMEM)],
        out_shape=[jax.ShapeDtypeStruct((D, D), F32)] * 4 + [jax.ShapeDtypeStruct((T, D), BF)],
        scratch_shapes=[pltpu.VMEM((2, 2, STEPS, LANE, HALF), F32), pltpu.VMEM((2, 2, STEPS, LANE, HALF), F32), pltpu.VMEM((2, 2, 2, LANE, HALF), F32),
                        pltpu.VMEM((D, D), BF), pltpu.VMEM((D, D), BF), pltpu.VMEM((D, D), BF),
                        sem(7), sem(7), sem(8), sem(8), sem(7), sem(7), sem(8), sem(8), pltpu.SemaphoreType.DMA((2, 2)), pltpu.SemaphoreType.DMA((3,))],
        compiler_params=pltpu.CompilerParams(has_side_effects=True, vmem_limit_bytes=63 * MIB),
       cost_estimate=cost(110),
    )(xt, att, dq, dk, dv, dyp, wq, wk, wv)


def finish_kernel(a_ref, b_ref, c_ref, d_ref, dxp_ref, a_out, b_out, c_out, d_out, dx_ref):
    j = pl.program_id(0)
    for src, dst in ((a_ref, a_out), (b_ref, b_out), (c_ref, c_out), (d_ref, d_out)):
        dst[...] = src[...]

    @pl.when(j < T // LANE)
    def _():
        z = jnp.concatenate([dxp_ref[pl.ds(pl.multiple_of(c * CH + 16 * j, 16), 16), :] for c in range(8)], axis=0)
        dx_ref[...] = dot(perm_matrix(True), z).astype(BF)


def finish_stage(a, b, c, d, dxp):
    block = pl.BlockSpec((LANE, D), lambda j: (j, 0))
    return pl.pallas_call(
        finish_kernel, grid=(8,), name='finish_stage',
        in_specs=[block] * 4 + [pl.BlockSpec((T, D), lambda j: (0, 0))],
        out_specs=[block] * 4 + [pl.BlockSpec((LANE, D), lambda j: (jnp.minimum(j, T // LANE - 1), 0))],
        out_shape=[jax.ShapeDtypeStruct((D, D), F32)] * 4 + [jax.ShapeDtypeStruct((T, D), BF)],
        compiler_params=pltpu.CompilerParams(vmem_limit_bytes=63 * MIB),
       cost_estimate=cost(2),
    )(a, b, c, d, dxp)


def solution(mesh):
    sp_size = mesh.shape['sp']

    def swap(a, bit):
        return lax.ppermute(a, 'sp', [(i, i ^ bit) for i in range(sp_size)])

    def device_work(x, w_q, w_k, w_v, w_o, dy):
        xt, dyp, q, k, v, do, sel = project(x, dy, w_q, w_k, w_v, w_o)
        sel8 = sel[:, ROWS:HALO]
        h2 = swap(sel8, 2)
        h1 = swap(sel, 1)
        h2, q = lax.optimization_barrier((h2, q))
        h3 = swap(h2, 1)
        grads, r1, r2 = (), [], []
        for half in range(2):
            *grads, one, two, three = attention(half, tuple(grads), q, k, v, do, h1, h2, h3)
            two = two + swap(three, 1)
            one, two, grads[0] = lax.optimization_barrier((one, two, grads[0]))
            r2.append(swap(two, 2))
            r1.append(swap(one, 1))
        at, dq, dk, dv = (g.reshape(T, D) for g in grads)
        y, att = out_stage(at, w_o)
        dkb, dvb = in_stage(dk, dv, *r1, *r2)
        dw_o, dw_q, dw_k, dw_v, dx = finish_stage(*ring_stage(xt, att, dq, dkb, dvb, dyp, w_q, w_k, w_v))
        return y, dx, dw_q, dw_k, dw_v, dw_o

    row_spec = P(('dp', 'sp'), None)
    full_spec = P(None, None)
    grad_spec = P('dp', None)
    return jax.shard_map(device_work, mesh=mesh, in_specs=(row_spec, full_spec, full_spec, full_spec, full_spec, row_spec), out_specs=(row_spec, row_spec, grad_spec, grad_spec, grad_spec, grad_spec), check_vma=False)
```
